8 devices in a mesh: dp: 1 (over z), tp: 2 (over y), ctx: 4 (over x, core).
Axes of the slice: x: 2, y: 2, z: 1, core: 2. Of those that a mesh axis runs over, the one named last changes fastest.
Arguments:
- hidden: bfloat16 [512, 5120], P(('dp', 'ctx'))
- w_q: bfloat16 [5120, 5120], P(None, 'tp')
- w_k: bfloat16 [5120, 1024], P(None, 'tp')
- w_v: bfloat16 [5120, 1024], P(None, 'tp')
- w_o: bfloat16 [5120, 5120], P('tp')
- k_prefix: bfloat16 [1024, 8, 128], P(('dp', 'ctx'), 'tp')
- v_prefix: bfloat16 [1024, 8, 128], P(('dp', 'ctx'), 'tp')
- k_suffix: bfloat16 [512, 256, 8, 128], P(('dp', 'ctx'), None, 'tp')
- v_suffix: bfloat16 [512, 256, 8, 128], P(('dp', 'ctx'), None, 'tp')
- seq_lens: int32 [512], P(('dp', 'ctx'))
Outputs:
- output: bfloat16 [512, 5120], P(('dp', 'ctx'))
All inputs are finite; a program needn't handle non-finite values.
Results may differ from the reference program's by a relative error of at most 0.0049065.
Values are sent between devices in bfloat16 or wider.
A program may use at most 1 GiB of HBM per device.

```python
import math
import jax
import jax.numpy as jnp
from jax import lax

NUM_SEQS = 512
PREFIX_LEN = 1024
SUFFIX_LEN = 256
MODEL_DIM = 5120
NUM_HEADS = 40
KV_HEADS = 8
HEAD_DIM = 128
GROUP_SIZE = NUM_HEADS // KV_HEADS


def setup_inputs(seed: int = 0, part: int = 0) -> dict:
    root_key = jax.random.key(seed)
    part_key = jax.random.fold_in(root_key, part)
    weight_keys = jax.random.split(root_key, 4)
    draw_keys = jax.random.split(part_key, 10)
    topic_count = 16
    log_ratio = min(max(math.log(2.0 * PREFIX_LEN / (topic_count * SUFFIX_LEN)), -3.0), 3.0)
    amp_prefix = 2.0 + max(-log_ratio, 0.0)
    amp_suffix = 3.0 + max(log_ratio, 0.0)
    q_cols = NUM_HEADS * HEAD_DIM
    kv_cols = KV_HEADS * HEAD_DIM
    in_scale = MODEL_DIM ** -0.5
    w_q = jax.random.normal(weight_keys[0], (MODEL_DIM, q_cols), jnp.float32) * in_scale
    lead_cols = w_q.reshape(MODEL_DIM, KV_HEADS, GROUP_SIZE, HEAD_DIM)[:, :, 0, :].reshape(MODEL_DIM, kv_cols)
    w_k = 0.6 * lead_cols + 0.8 * in_scale * jax.random.normal(weight_keys[1], (MODEL_DIM, kv_cols), jnp.float32)
    w_v = in_scale * jax.random.normal(weight_keys[2], (MODEL_DIM, kv_cols), jnp.float32)
    w_o = jax.random.normal(weight_keys[3], (q_cols, MODEL_DIM), jnp.float32) * q_cols ** -0.5
    hidden = jax.random.normal(draw_keys[0], (NUM_SEQS, MODEL_DIM), jnp.float32)
    topic_hid = jax.random.normal(draw_keys[1], (topic_count, MODEL_DIM), jnp.float32)
    topic_key = jnp.dot(topic_hid, w_k).reshape(topic_count, KV_HEADS, HEAD_DIM)
    topic_val = jnp.dot(topic_hid, w_v).reshape(topic_count, KV_HEADS, HEAD_DIM)
    pos_topic = jnp.arange(PREFIX_LEN) * topic_count // PREFIX_LEN
    kv_shape = (PREFIX_LEN, KV_HEADS, HEAD_DIM)
    k_prefix = amp_prefix * topic_key[pos_topic] + jax.random.normal(draw_keys[2], kv_shape, jnp.float32)
    v_prefix = topic_val[pos_topic] + 0.5 * jax.random.normal(draw_keys[3], kv_shape, jnp.float32)
    own_hid = jax.random.normal(draw_keys[4], (NUM_SEQS, MODEL_DIM), jnp.float32)
    stale_hid = jax.random.normal(draw_keys[5], (NUM_SEQS, MODEL_DIM), jnp.float32)
    head_shape = (NUM_SEQS, 1, KV_HEADS, HEAD_DIM)
    own_key = jnp.dot(own_hid, w_k).reshape(head_shape)
    own_val = jnp.dot(own_hid, w_v).reshape(head_shape)
    stale_key = jnp.dot(stale_hid, w_k).reshape(head_shape)
    stale_val = jnp.dot(stale_hid, w_v).reshape(head_shape)
    seq_lens = jax.random.randint(draw_keys[6], (NUM_SEQS,), 0, SUFFIX_LEN)
    seq_lens = seq_lens.at[0].set(SUFFIX_LEN - 1).at[NUM_SEQS - 1].set(0)
    in_use = (jnp.arange(SUFFIX_LEN)[None, :] < seq_lens[:, None])[:, :, None, None]
    suf_shape = (NUM_SEQS, SUFFIX_LEN, KV_HEADS, HEAD_DIM)
    k_suffix = amp_suffix * jnp.where(in_use, own_key, stale_key) + jax.random.normal(draw_keys[7], suf_shape, jnp.float32)
    v_suffix = jnp.where(in_use, own_val, stale_val) + 0.5 * jax.random.normal(draw_keys[8], suf_shape, jnp.float32)
    return dict(hidden=hidden.astype(jnp.bfloat16), w_q=w_q.astype(jnp.bfloat16), w_k=w_k.astype(jnp.bfloat16), w_v=w_v.astype(jnp.bfloat16), w_o=w_o.astype(jnp.bfloat16), k_prefix=k_prefix.astype(jnp.bfloat16), v_prefix=v_prefix.astype(jnp.bfloat16), k_suffix=k_suffix.astype(jnp.bfloat16), v_suffix=v_suffix.astype(jnp.bfloat16), seq_lens=seq_lens)


def reference(hidden, w_q, w_k, w_v, w_o, k_prefix, v_prefix, k_suffix, v_suffix, seq_lens):
    q_all = jnp.dot(hidden, w_q, preferred_element_type=jnp.float32).astype(jnp.bfloat16)
    k_new = jnp.dot(hidden, w_k, preferred_element_type=jnp.float32).astype(jnp.bfloat16)
    v_new = jnp.dot(hidden, w_v, preferred_element_type=jnp.float32).astype(jnp.bfloat16)
    slot_ids = jnp.arange(SUFFIX_LEN)
    at_new = (slot_ids[None, :] == seq_lens[:, None])[:, :, None, None]
    k_cur = jnp.where(at_new, k_new.reshape(NUM_SEQS, 1, KV_HEADS, HEAD_DIM), k_suffix).astype(jnp.float32)
    v_cur = jnp.where(at_new, v_new.reshape(NUM_SEQS, 1, KV_HEADS, HEAD_DIM), v_suffix).astype(jnp.float32)
    visible = slot_ids[None, :] <= seq_lens[:, None]
    q_grp = q_all.astype(jnp.float32).reshape(NUM_SEQS, KV_HEADS, GROUP_SIZE, HEAD_DIM)
    k_pre32 = k_prefix.astype(jnp.float32)
    v_pre32 = v_prefix.astype(jnp.float32)
    score_scale = HEAD_DIM ** -0.5

    def one_sequence(seq_items):
        q_one, k_one, v_one, vis_one = seq_items
        s_pre = jnp.einsum('kgd,pkd->kgp', q_one, k_pre32) * score_scale
        s_suf = jnp.einsum('kgd,skd->kgs', q_one, k_one) * score_scale
        s_suf = jnp.where(vis_one[None, None, :], s_suf, -jnp.inf)
        run_max = jnp.maximum(jnp.max(s_pre, axis=-1), jnp.max(s_suf, axis=-1))[..., None]
        e_pre = jnp.exp(s_pre - run_max)
        e_suf = jnp.exp(s_suf - run_max)
        weight_sum = jnp.sum(e_pre, axis=-1) + jnp.sum(e_suf, axis=-1)
        weighted = jnp.einsum('kgp,pkd->kgd', e_pre, v_pre32) + jnp.einsum('kgs,skd->kgd', e_suf, v_one)
        return weighted / weight_sum[..., None]

    attn_out = lax.map(one_sequence, (q_grp, k_cur, v_cur, visible))
    attn_out = attn_out.reshape(NUM_SEQS, NUM_HEADS * HEAD_DIM).astype(jnp.bfloat16)
    out_hidden = hidden.astype(jnp.float32) + jnp.dot(attn_out, w_o, preferred_element_type=jnp.float32)
    return out_hidden.astype(jnp.bfloat16)
```

```python
import functools

import jax
import jax.numpy as jnp
from jax import lax
from jax.experimental import pallas as pl
from jax.experimental.pallas import tpu as pltpu
from jax.sharding import PartitionSpec as P

MESH = pl.DeviceIdType.MESH
F32 = jnp.float32
BF16 = jnp.bfloat16
LOG2E = 1.4426950408889634
LOW = -3.0e38

CB = 512
SUB = 32
GRP = 8
RING = 3
PAD = 24


def mm(a, b):
    return jnp.dot(a, b, preferred_element_type=F32)


def mmt(a, b):
    return lax.dot_general(a, b, (((1,), (1,)), ((), ())), preferred_element_type=F32)


def body(dims, hid, wq, wk, wv, wo, kp, vp, ks, vs, lens, out,
         x_v, xo_v, wo_v, k_ring, v_ring, q2, qg, kn, vn, pre, dei, kvp, key,
         o2, m2, l2, att, snd, rcv, own, yo, yp,
         x_sem, p_sem, w_sem, wo_sem, kv_sem, g_snd, g_rcv, f_snd, f_rcv, y_snd, y_rcv, o_sem):
    nseq, model, heads, kvh, hd, slots = dims
    grp_heads = heads // kvh
    rows = slots * kvh
    half = model // 2
    nq = heads * hd // CB
    nh = half // CB
    nsub = nseq // SUB
    ngrp = nseq // GRP
    gps = SUB // GRP
    kdim = heads * hd
    c = lax.axis_index('ctx')
    t = lax.axis_index('tp')
    far = {'ctx': lax.rem(c + 2, 4)}
    near = {'ctx': c + 1 - 2 * lax.rem(c, 2)}
    mate = {'tp': 1 - t}
    cs = LOG2E * hd ** -0.5

    def remote(src, dst, ss, rs, dev):
        return pltpu.make_async_remote_copy(src_ref=src, dst_ref=dst, send_sem=ss, recv_sem=rs,
                                            device_id=dev, device_id_type=MESH)

    def w_copies(src, col, slot):
        return [pltpu.make_async_copy(src.at[pl.ds(i * kdim, kdim), pl.ds(col, CB)],
                                      wo_v.at[2 * slot + i], w_sem.at[slot, i]) for i in range(2)]

    def w_start(src, col, slot):
        for cp in w_copies(src, col, slot):
            cp.start()

    def wo_copy(j):
        col = jnp.where(j < nh, (1 - t) * half, t * half - half) + j * CB
        return pltpu.make_async_copy(wo.at[:, pl.ds(pl.multiple_of(col, CB), CB)], wo_v.at[j], wo_sem.at[j])

    def kv_copies(g):
        slot = lax.rem(g, RING)
        src = pl.ds(g * GRP * rows, GRP * rows)
        return [pltpu.make_async_copy(ks.at[src], k_ring.at[slot], kv_sem.at[slot, 0]),
                pltpu.make_async_copy(vs.at[src], v_ring.at[slot], kv_sem.at[slot, 1])]

    def kv_start(g):
        for cp in kv_copies(g):
            cp.start()

    x_copy = pltpu.make_async_copy(hid, x_v, x_sem.at[0])
    xo_copy = pltpu.make_async_copy(hid.at[:, pl.ds(pl.multiple_of(t * half, CB), half)], xo_v, x_sem.at[1])
    p_copies = [pltpu.make_async_copy(kp, pre.at[0], p_sem.at[0]), pltpu.make_async_copy(vp, pre.at[1], p_sem.at[1])]
    p_copies[0].start()
    p_copies[1].start()
    x_copy.start()
    for n in range(RING):
        w_start(wq, n * CB, n)
    xo_copy.start()

    barrier = pltpu.get_barrier_semaphore()
    for dev in (far, near, mate):
        pl.semaphore_signal(barrier, inc=1, device_id=dev, device_id_type=MESH)

    for i in range(2):
        p_copies[i].wait()
        dei[...] = pre[i].astype(F32)
        for h in range(kvh):
            kvp[0, i, h] = dei[pl.ds(h, kvp.shape[3], stride=kvh), :].astype(BF16)
    pl.semaphore_wait(barrier, 3)
    to_far = remote(kvp.at[0], kvp.at[2], g_snd.at[0], g_rcv.at[0], far)
    to_near = remote(kvp.at[0], kvp.at[1], g_snd.at[1], g_rcv.at[1], near)
    pass_on = remote(kvp.at[2], kvp.at[3], g_snd.at[2], g_rcv.at[2], near)
    to_far.start()
    to_near.start()

    row_head = lax.broadcasted_iota(jnp.int32, (PAD, rows), 0) // grp_heads
    col_row = lax.broadcasted_iota(jnp.int32, (PAD, rows), 1)
    key[...] = jnp.where(lax.rem(col_row, kvh) == row_head, col_row // kvh, slots)
    for h in range(heads, PAD):
        q2[pl.ds(h, nseq, stride=PAD), :] = jnp.zeros((nseq, hd), F32)

    x_copy.wait()

    def project(slot):
        return mm(x_v[:, :kdim], wo_v[2 * slot]) + mm(x_v[:, kdim:], wo_v[2 * slot + 1])

    hpb = CB // hd

    def q_block(n, carry):
        slot = lax.rem(n, RING)
        for cp in w_copies(wq, pl.multiple_of(n * CB, CB), slot):
            cp.wait()
        q = project(slot).astype(BF16)
        for i in range(hpb):
            one = q[:, i * hd:(i + 1) * hd]
            qg[hpb * n + i] = one
            q2[pl.ds(hpb * n + i, nseq, stride=PAD), :] = one.astype(F32)

        @pl.when(n + RING < nq)
        def _():
            w_start(wq, pl.multiple_of((n + RING) * CB, CB), slot)

        @pl.when(n + RING == nq)
        def _():
            w_start(wk, 0, slot)

        @pl.when(n + RING == nq + 1)
        def _():
            w_start(wv, 0, slot)
            kv_start(0)

        @pl.when(n + RING == nq + 2)
        def _():
            kv_start(1)
        return carry

    lax.fori_loop(0, nq, q_block, 0)
    for n, src, dst in ((nq, wk, kn), (nq + 1, wv, vn)):
        for cp in w_copies(src, 0, n % RING):
            cp.wait()
        new = project(n % RING).astype(BF16).astype(F32)
        for h in range(kvh):
            dst[h] = new[:, h * hd:(h + 1) * hd]
        if n == nq:
            kv_start(2)
    xo_copy.wait()

    zero8 = jnp.zeros((8, hd), F32)
    zero32 = jnp.zeros((32, hd), BF16)
    quarter = rows // 4

    def attend(g):
        slot = lax.rem(g, RING)
        for i in range(GRP):
            b = g * GRP + i
            q = q2[pl.ds(pl.multiple_of(b * PAD, 8), PAD), :]
            q = jnp.concatenate([q, zero8], 0).astype(BF16)
            lhs = jnp.concatenate([jnp.concatenate([q, zero32], 1), jnp.concatenate([zero32, q], 1)], 0)
            base = i * rows
            s = []
            for p in range(2):
                k0 = k_ring[slot, base + 2 * p * quarter:base + (2 * p + 1) * quarter, :]
                k1 = k_ring[slot, base + (2 * p + 1) * quarter:base + (2 * p + 2) * quarter, :]
                r = mmt(lhs, jnp.concatenate([k0, k1], 1))
                s += [r[0:PAD], r[32:32 + PAD]]
            n_old = lens[b]
            s = [jnp.where(key[:, p * quarter:(p + 1) * quarter] < n_old, s[p], -jnp.inf) for p in range(4)]
            m = jnp.maximum(jnp.maximum(s[0], s[1]), jnp.maximum(s[2], s[3]))
            m = jnp.maximum(jnp.max(m, axis=1, keepdims=True), LOW)
            e = [jnp.exp2((a - m) * cs) for a in s]
            l = jnp.sum((e[0] + e[1]) + (e[2] + e[3]), axis=1, keepdims=True)
            gap = jnp.zeros((8, 2 * quarter), F32)
            w = jnp.concatenate([jnp.concatenate([e[0], e[2]], 1), gap,
                                 jnp.concatenate([e[1], e[3]], 1), gap], 0).astype(BF16)
            v = [v_ring[slot, base + p * quarter:base + (p + 1) * quarter, :] for p in range(4)]
            v = jnp.concatenate([jnp.concatenate([v[0], v[1]], 1), jnp.concatenate([v[2], v[3]], 1)], 0)
            o = mm(w, v)
            at = pl.ds(pl.multiple_of(lax.rem(b, SUB) * PAD, 8), PAD)
            o2[at, :] = o[0:PAD, :hd] + o[32:32 + PAD, hd:]
            m2[at, :] = jnp.broadcast_to(m, (PAD, hd))
            l2[at, :] = jnp.broadcast_to(l, (PAD, hd))

    def group(g, carry):
        for cp in kv_copies(g):
            cp.wait()
        attend(g)

        @pl.when(jnp.logical_or(g == 0, jnp.logical_and(g >= gps, g + RING < ngrp)))
        def _():
            kv_start(g + RING)

        wo_steps = [(0, 2), (2, 5), (5, 8), (8, 2 * nh)]
        for n, (lo, hi) in enumerate(wo_steps):
            @pl.when(g == n)
            def _():
                for j in range(lo, hi):
                    wo_copy(j).start()

        @pl.when(g == gps - 1)
        def _():
            for n in range(gps, gps + RING):
                kv_start(n)

        @pl.when(g == 1)
        def _():
            to_far.wait_recv()
            pass_on.start()
        return carry

    def merge(s, h):
        at = pl.ds(pl.multiple_of(s * SUB, SUB), SUB)
        q = qg[pl.ds(h * grp_heads, grp_heads), at, :].reshape(grp_heads * SUB, hd)
        sc = [mmt(q, kvp[n, 0, h]) for n in range(4)]
        m = jnp.maximum(jnp.maximum(sc[0], sc[1]), jnp.maximum(sc[2], sc[3]))
        m = jnp.max(m, axis=1, keepdims=True)
        e = [jnp.exp2((a - m) * cs) for a in sc]
        l = jnp.sum((e[0] + e[1]) + (e[2] + e[3]), axis=1, keepdims=True)
        o = mm(jnp.concatenate([a.astype(BF16) for a in e], 1),
               jnp.concatenate([kvp[n, 1, h] for n in range(4)], 0))
        k_new = kn[h, at, :]
        v_new = vn[h, at, :]
        for i in range(grp_heads):
            part = slice(i * SUB, (i + 1) * SUB)
            rows_at = pl.ds(h * grp_heads + i, SUB, stride=PAD)
            m_s, l_s, o_s = m2[rows_at, :], l2[rows_at, :], o2[rows_at, :]
            s_n = jnp.sum(q[part].astype(F32) * k_new, axis=1, keepdims=True)
            m_p = jnp.maximum(m[part], s_n)
            m_all = jnp.maximum(m_p, m_s)
            w_p = jnp.exp2((m[part] - m_all) * cs)
            w_n = jnp.exp2((s_n - m_all) * cs)
            w_s = jnp.exp2((m_s - m_all) * cs)
            total = w_p * l[part] + w_n + w_s * l_s
            val = (w_p * o[part] + w_n * v_new + w_s * o_s) / total
            att[h * grp_heads + i] = val.astype(BF16)

    def a_rows():
        return jnp.concatenate([att[h] for h in range(heads)], 1)

    def partial_copy(s, j):
        return remote(snd.at[s, j], rcv.at[s, j], f_snd.at[s, j], f_rcv.at[s, j], mate)

    def y_copy(s, j):
        return remote(yo.at[s, j], yp.at[s, j], y_snd.at[s, j], y_rcv.at[s, j], mate)

    def out_copy(src, which, s, j):
        side = t if which == 0 else 1 - t
        col = pl.multiple_of(side * half + j * CB, CB)
        return pltpu.make_async_copy(src.at[s, j], out.at[pl.ds(pl.multiple_of(s * SUB, SUB), SUB), pl.ds(col, CB)],
                                     o_sem.at[which, s, j])

    def finish(s):
        def step(j, carry):
            partial_copy(s, j).wait_recv()
            yo[s, j] = (own[s, j] + rcv[s, j]).astype(BF16)
            y_copy(s, j).start()
            out_copy(yo, 0, s, j).start()
            return carry
        lax.fori_loop(0, nh, step, 0)

    def sub_pass(s, carry):
        lax.fori_loop(s * gps, (s + 1) * gps, group, 0)

        @pl.when(s == 0)
        def _():
            to_near.wait_recv()
            pass_on.wait_recv()

        def one_head(h, cc):
            merge(s, h)
            return cc
        lax.fori_loop(0, kvh, one_head, 0)

        def send(j, cc):
            @pl.when(s == 0)
            def _():
                wo_copy(j).wait()
            snd[s, j] = mm(a_rows(), wo_v[j])
            partial_copy(s, j).start()
            return cc
        lax.fori_loop(0, nh, send, 0)

        def keep(j, cc):
            @pl.when(s == 0)
            def _():
                wo_copy(nh + j).wait()
            x_at = xo_v[pl.ds(pl.multiple_of(s * SUB, SUB), SUB), pl.ds(pl.multiple_of(j * CB, CB), CB)]
            own[s, j] = mm(a_rows(), wo_v[nh + j]) + x_at.astype(F32)
            return cc
        lax.fori_loop(0, nh, keep, 0)

        @pl.when(s > 0)
        def _():
            finish(s - 1)
        return carry

    lax.fori_loop(0, nsub, sub_pass, 0)
    finish(nsub - 1)

    def tail(n, carry):
        s, j = n // nh, lax.rem(n, nh)
        y_copy(s, j).wait_recv()
        out_copy(yp, 1, s, j).start()
        return carry
    lax.fori_loop(0, nsub * nh, tail, 0)

    def drain(n, carry):
        s, j = n // nh, lax.rem(n, nh)
        partial_copy(s, j).wait_send()
        y_copy(s, j).wait_send()
        out_copy(yo, 0, s, j).wait()
        out_copy(yp, 1, s, j).wait()
        return carry
    lax.fori_loop(0, nsub * nh, drain, 0)
    to_far.wait_send()
    to_near.wait_send()
    pass_on.wait_send()


def solution(mesh):
    row_axes = ('dp', 'ctx')

    def device_step(hidden, w_q, w_k, w_v, w_o, k_prefix, v_prefix, k_suffix, v_suffix, seq_lens):
        nseq, model = hidden.shape
        npos, kvh, hd = k_prefix.shape
        slots = k_suffix.shape[1]
        heads = w_q.shape[1] // hd
        rows = slots * kvh
        nsub, nh = nseq // SUB, model // 2 // CB
        dims = (nseq, model, heads, kvh, hd, slots)
        hbm = pl.BlockSpec(memory_space=pl.ANY)
        dma = pltpu.SemaphoreType.DMA
        return pl.pallas_call(
            functools.partial(body, dims),
            out_shape=jax.ShapeDtypeStruct((nseq, model), BF16),
            in_specs=[hbm] * 9 + [pl.BlockSpec(memory_space=pltpu.SMEM)],
            out_specs=hbm,
            scratch_shapes=[
                pltpu.VMEM((nseq, model), BF16),
                pltpu.VMEM((nseq, model // 2), BF16),
                pltpu.VMEM((2 * nh, heads * hd, CB), BF16),
                pltpu.VMEM((RING, GRP * rows, hd), BF16),
                pltpu.VMEM((RING, GRP * rows, hd), BF16),
                pltpu.VMEM((nseq * PAD, hd), F32),
                pltpu.VMEM((heads, nseq, hd), BF16),
                pltpu.VMEM((kvh, nseq, hd), F32),
                pltpu.VMEM((kvh, nseq, hd), F32),
                pltpu.VMEM((2, npos * kvh, hd), BF16),
                pltpu.VMEM((npos * kvh, hd), F32),
                pltpu.VMEM((4, 2, kvh, npos, hd), BF16),
                pltpu.VMEM((PAD, rows), jnp.int32),
                pltpu.VMEM((SUB * PAD, hd), F32),
                pltpu.VMEM((SUB * PAD, hd), F32),
                pltpu.VMEM((SUB * PAD, hd), F32),
                pltpu.VMEM((heads, SUB, hd), BF16),
                pltpu.VMEM((nsub, nh, SUB, CB), F32),
                pltpu.VMEM((nsub, nh, SUB, CB), F32),
                pltpu.VMEM((nsub, nh, SUB, CB), F32),
                pltpu.VMEM((nsub, nh, SUB, CB), BF16),
                pltpu.VMEM((nsub, nh, SUB, CB), BF16),
                dma((2,)), dma((2,)), dma((RING, 2)), dma((2 * nh,)), dma((RING, 2)),
                dma((3,)), dma((3,)), dma((nsub, nh)), dma((nsub, nh)), dma((nsub, nh)), dma((nsub, nh)),
                dma((2, nsub, nh)),
            ],
            compiler_params=pltpu.CompilerParams(collective_id=0, has_side_effects=True,
                                                 vmem_limit_bytes=67043328),
        )(hidden, w_q, w_k, w_v, w_o,
          k_prefix.reshape(npos * kvh, hd), v_prefix.reshape(npos * kvh, hd),
          k_suffix.reshape(nseq * rows, hd), v_suffix.reshape(nseq * rows, hd), seq_lens)

    spec_in = (P(row_axes, None), P(None, 'tp'), P(None, 'tp'), P(None, 'tp'), P('tp', None), P(row_axes, 'tp', None), P(row_axes, 'tp', None), P(row_axes, None, 'tp', None), P(row_axes, None, 'tp', None), P(row_axes))
    return jax.shard_map(device_step, mesh=mesh, in_specs=spec_in, out_specs=P(row_axes, None), check_vma=False)
```

```python
import functools

import jax
import jax.numpy as jnp
from jax import lax
from jax.experimental import pallas as pl
from jax.experimental.pallas import tpu as pltpu
from jax.sharding import PartitionSpec as P

MESH = pl.DeviceIdType.MESH
F32 = jnp.float32
BF16 = jnp.bfloat16
LOG2E = 1.4426950408889634
LOW = -3.0e38

CB = 512
SUB = 32
GRP = 8
RING = 3
PAD = 24


def mm(a, b):
    return jnp.dot(a, b, preferred_element_type=F32)


def mmt(a, b):
    return lax.dot_general(a, b, (((1,), (1,)), ((), ())), preferred_element_type=F32)


def body(dims, hid, wq, wk, wv, wo, kp, vp, ks, vs, lens, out,
         x_v, xo_v, wo_v, k_ring, v_ring, q2, qg, kn, vn, pre, dei, kvp, key,
         o2, m2, l2, att, snd, rcv, own, yo, yp,
         x_sem, p_sem, w_sem, wo_sem, kv_sem, g_snd, g_rcv, f_snd, f_rcv, y_snd, y_rcv, o_sem):
    nseq, model, heads, kvh, hd, slots = dims
    grp_heads = heads // kvh
    rows = slots * kvh
    half = model // 2
    nq = heads * hd // CB
    nh = half // CB
    nsub = nseq // SUB
    ngrp = nseq // GRP
    gps = SUB // GRP
    kdim = heads * hd
    c = lax.axis_index('ctx')
    t = lax.axis_index('tp')
    far = {'ctx': lax.rem(c + 2, 4)}
    near = {'ctx': c + 1 - 2 * lax.rem(c, 2)}
    mate = {'tp': 1 - t}
    cs = LOG2E * hd ** -0.5

    def remote(src, dst, ss, rs, dev):
        return pltpu.make_async_remote_copy(src_ref=src, dst_ref=dst, send_sem=ss, recv_sem=rs,
                                            device_id=dev, device_id_type=MESH)

    def w_copies(src, col, slot):
        return [pltpu.make_async_copy(src.at[pl.ds(i * kdim, kdim), pl.ds(col, CB)],
                                      wo_v.at[2 * slot + i], w_sem.at[slot, i]) for i in range(2)]

    def w_start(src, col, slot):
        for cp in w_copies(src, col, slot):
            cp.start()

    def wo_copy(j):
        col = jnp.where(j < nh, (1 - t) * half, t * half - half) + j * CB
        return pltpu.make_async_copy(wo.at[:, pl.ds(pl.multiple_of(col, CB), CB)], wo_v.at[j], wo_sem.at[j])

    def kv_copies(g):
        slot = lax.rem(g, RING)
        src = pl.ds(g * GRP * rows, GRP * rows)
        return [pltpu.make_async_copy(ks.at[src], k_ring.at[slot], kv_sem.at[slot, 0]),
                pltpu.make_async_copy(vs.at[src], v_ring.at[slot], kv_sem.at[slot, 1])]

    def kv_start(g):
        for cp in kv_copies(g):
            cp.start()

    x_copy = pltpu.make_async_copy(hid, x_v, x_sem.at[0])
    xo_copy = pltpu.make_async_copy(hid.at[:, pl.ds(pl.multiple_of(t * half, CB), half)], xo_v, x_sem.at[1])
    p_copies = [pltpu.make_async_copy(kp, pre.at[0], p_sem.at[0]), pltpu.make_async_copy(vp, pre.at[1], p_sem.at[1])]
    p_copies[0].start()
    p_copies[1].start()
    x_copy.start()
    for n in range(RING):
        w_start(wq, n * CB, n)
    xo_copy.start()

    barrier = pltpu.get_barrier_semaphore()
    for dev in (far, near, mate):
        pl.semaphore_signal(barrier, inc=1, device_id=dev, device_id_type=MESH)

    for i in range(2):
        p_copies[i].wait()
        dei[...] = pre[i].astype(F32)
        for h in range(kvh):
            kvp[0, i, h] = dei[pl.ds(h, kvp.shape[3], stride=kvh), :].astype(BF16)
    pl.semaphore_wait(barrier, 3)
    to_far = remote(kvp.at[0], kvp.at[2], g_snd.at[0], g_rcv.at[0], far)
    to_near = remote(kvp.at[0], kvp.at[1], g_snd.at[1], g_rcv.at[1], near)
    pass_on = remote(kvp.at[2], kvp.at[3], g_snd.at[2], g_rcv.at[2], near)
    to_far.start()
    to_near.start()

    row_head = lax.broadcasted_iota(jnp.int32, (PAD, rows), 0) // grp_heads
    col_row = lax.broadcasted_iota(jnp.int32, (PAD, rows), 1)
    key[...] = jnp.where(lax.rem(col_row, kvh) == row_head, col_row // kvh, slots)
    for h in range(heads, PAD):
        q2[pl.ds(h, nseq, stride=PAD), :] = jnp.zeros((nseq, hd), F32)

    x_copy.wait()

    def project(slot):
        return mm(x_v[:, :kdim], wo_v[2 * slot]) + mm(x_v[:, kdim:], wo_v[2 * slot + 1])

    hpb = CB // hd

    def q_block(n, carry):
        slot = lax.rem(n, RING)
        for cp in w_copies(wq, pl.multiple_of(n * CB, CB), slot):
            cp.wait()
        q = project(slot).astype(BF16)
        for i in range(hpb):
            one = q[:, i * hd:(i + 1) * hd]
            qg[hpb * n + i] = one
            q2[pl.ds(hpb * n + i, nseq, stride=PAD), :] = one.astype(F32)

        @pl.when(n + RING < nq)
        def _():
            w_start(wq, pl.multiple_of((n + RING) * CB, CB), slot)

        @pl.when(n + RING == nq)
        def _():
            w_start(wk, 0, slot)

        @pl.when(n + RING == nq + 1)
        def _():
            w_start(wv, 0, slot)
            kv_start(0)

        @pl.when(n + RING == nq + 2)
        def _():
            kv_start(1)
        return carry

    lax.fori_loop(0, nq, q_block, 0)
    for n, src, dst in ((nq, wk, kn), (nq + 1, wv, vn)):
        for cp in w_copies(src, 0, n % RING):
            cp.wait()
        new = project(n % RING).astype(BF16).astype(F32)
        for h in range(kvh):
            dst[h] = new[:, h * hd:(h + 1) * hd]
        if n == nq:
            kv_start(2)
    xo_copy.wait()

    zero8 = jnp.zeros((8, hd), F32)
    zero32 = jnp.zeros((32, hd), BF16)
    quarter = rows // 4

    def scores(slot, b, base):
        q = q2[pl.ds(pl.multiple_of(b * PAD, 8), PAD), :]
        q = jnp.concatenate([q, zero8], 0).astype(BF16)
        lhs = jnp.concatenate([jnp.concatenate([q, zero32], 1), jnp.concatenate([zero32, q], 1)], 0)
        s = []
        for p in range(2):
            k0 = k_ring[slot, base + 2 * p * quarter:base + (2 * p + 1) * quarter, :]
            k1 = k_ring[slot, base + (2 * p + 1) * quarter:base + (2 * p + 2) * quarter, :]
            r = mmt(lhs, jnp.concatenate([k0, k1], 1))
            s += [r[0:PAD], r[32:32 + PAD]]
        return s

    def weights(s, b):
        n_old = lens[b]
        s = [jnp.where(key[:, p * quarter:(p + 1) * quarter] < n_old, s[p], -jnp.inf) for p in range(4)]
        m = jnp.maximum(jnp.maximum(s[0], s[1]), jnp.maximum(s[2], s[3]))
        m = jnp.maximum(jnp.max(m, axis=1, keepdims=True), LOW)
        e = [jnp.exp2((a - m) * cs) for a in s]
        l = jnp.sum((e[0] + e[1]) + (e[2] + e[3]), axis=1, keepdims=True)
        gap = jnp.zeros((8, 2 * quarter), F32)
        w = jnp.concatenate([jnp.concatenate([e[0], e[2]], 1), gap,
                             jnp.concatenate([e[1], e[3]], 1), gap], 0).astype(BF16)
        at = pl.ds(pl.multiple_of(lax.rem(b, SUB) * PAD, 8), PAD)
        m2[at, :] = jnp.broadcast_to(m, (PAD, hd))
        l2[at, :] = jnp.broadcast_to(l, (PAD, hd))
        return w

    def values(w, slot, b, base):
        v = [v_ring[slot, base + p * quarter:base + (p + 1) * quarter, :] for p in range(4)]
        v = jnp.concatenate([jnp.concatenate([v[0], v[1]], 1), jnp.concatenate([v[2], v[3]], 1)], 0)
        o = mm(w, v)
        at = pl.ds(pl.multiple_of(lax.rem(b, SUB) * PAD, 8), PAD)
        o2[at, :] = o[0:PAD, :hd] + o[32:32 + PAD, hd:]

    def attend(g):
        slot = lax.rem(g, RING)
        s, w = {}, {}
        for n in range(GRP + 2):
            if n < GRP:
                s[n] = scores(slot, g * GRP + n, n * rows)
            if 0 <= n - 2 < GRP:
                values(w.pop(n - 2), slot, g * GRP + n - 2, (n - 2) * rows)
            if 0 <= n - 1 < GRP:
                w[n - 1] = weights(s.pop(n - 1), g * GRP + n - 1)

    def group(g, carry):
        for cp in kv_copies(g):
            cp.wait()
        attend(g)

        @pl.when(jnp.logical_or(g == 0, jnp.logical_and(g >= gps, g + RING < ngrp)))
        def _():
            kv_start(g + RING)

        wo_steps = [(0, 2), (2, 5), (5, 8), (8, 2 * nh)]
        for n, (lo, hi) in enumerate(wo_steps):
            @pl.when(g == n)
            def _():
                for j in range(lo, hi):
                    wo_copy(j).start()

        @pl.when(g == gps - 1)
        def _():
            for n in range(gps, gps + RING):
                kv_start(n)

        @pl.when(g == 1)
        def _():
            to_far.wait_recv()
            pass_on.start()
        return carry

    def merge(s):
        at = pl.ds(pl.multiple_of(s * SUB, SUB), SUB)

        def pre_scores(h):
            q = qg[h * grp_heads:(h + 1) * grp_heads, at, :].reshape(grp_heads * SUB, hd)
            return q, [mmt(q, kvp[n, 0, h]) for n in range(4)]

        def pre_weights(sc):
            m = jnp.maximum(jnp.maximum(sc[0], sc[1]), jnp.maximum(sc[2], sc[3]))
            m = jnp.max(m, axis=1, keepdims=True)
            e = [jnp.exp2((a - m) * cs) for a in sc]
            l = jnp.sum((e[0] + e[1]) + (e[2] + e[3]), axis=1, keepdims=True)
            return jnp.concatenate([a.astype(BF16) for a in e], 1), m, l

        def join(h, q, w, m, l):
            o = mm(w, jnp.concatenate([kvp[n, 1, h] for n in range(4)], 0))
            k_new = kn[h, at, :]
            v_new = vn[h, at, :]
            for i in range(grp_heads):
                part = slice(i * SUB, (i + 1) * SUB)
                rows_at = pl.ds(h * grp_heads + i, SUB, stride=PAD)
                m_s, l_s, o_s = m2[rows_at, :], l2[rows_at, :], o2[rows_at, :]
                s_n = jnp.sum(q[part].astype(F32) * k_new, axis=1, keepdims=True)
                m_p = jnp.maximum(m[part], s_n)
                m_all = jnp.maximum(m_p, m_s)
                w_p = jnp.exp2((m[part] - m_all) * cs)
                w_n = jnp.exp2((s_n - m_all) * cs)
                w_s = jnp.exp2((m_s - m_all) * cs)
                total = w_p * l[part] + w_n + w_s * l_s
                val = (w_p * o[part] + w_n * v_new + w_s * o_s) / total
                att[h * grp_heads + i] = val.astype(BF16)

        sc, w = {}, {}
        for n in range(kvh + 2):
            if n < kvh:
                sc[n] = pre_scores(n)
            if 0 <= n - 2 < kvh:
                join(n - 2, *w.pop(n - 2))
            if 0 <= n - 1 < kvh:
                q, p = sc.pop(n - 1)
                w[n - 1] = (q,) + pre_weights(p)

    def a_rows():
        return jnp.concatenate([att[h] for h in range(heads)], 1)

    def partial_copy(s, j):
        return remote(snd.at[s, j], rcv.at[s, j], f_snd.at[s, j], f_rcv.at[s, j], mate)

    def y_copy(s, j):
        return remote(yo.at[s, j], yp.at[s, j], y_snd.at[s, j], y_rcv.at[s, j], mate)

    def out_copy(src, which, s, j):
        side = t if which == 0 else 1 - t
        col = pl.multiple_of(side * half + j * CB, CB)
        return pltpu.make_async_copy(src.at[s, j], out.at[pl.ds(pl.multiple_of(s * SUB, SUB), SUB), pl.ds(col, CB)],
                                     o_sem.at[which, s, j])

    def finish(s):
        def step(j, carry):
            partial_copy(s, j).wait_recv()
            yo[s, j] = (own[s, j] + rcv[s, j]).astype(BF16)
            y_copy(s, j).start()
            out_copy(yo, 0, s, j).start()
            return carry
        lax.fori_loop(0, nh, step, 0)

    def sub_pass(s, carry):
        lax.fori_loop(s * gps, (s + 1) * gps, group, 0)

        @pl.when(s == 0)
        def _():
            to_near.wait_recv()
            pass_on.wait_recv()

        merge(s)

        def send(j, cc):
            @pl.when(s == 0)
            def _():
                wo_copy(j).wait()
            snd[s, j] = mm(a_rows(), wo_v[j])
            partial_copy(s, j).start()
            return cc
        lax.fori_loop(0, nh, send, 0)

        def keep(j, cc):
            @pl.when(s == 0)
            def _():
                wo_copy(nh + j).wait()
            x_at = xo_v[pl.ds(pl.multiple_of(s * SUB, SUB), SUB), pl.ds(pl.multiple_of(j * CB, CB), CB)]
            own[s, j] = mm(a_rows(), wo_v[nh + j]) + x_at.astype(F32)
            return cc
        lax.fori_loop(0, nh, keep, 0)

        @pl.when(s > 0)
        def _():
            finish(s - 1)
        return carry

    lax.fori_loop(0, nsub, sub_pass, 0)
    finish(nsub - 1)

    def tail(n, carry):
        s, j = n // nh, lax.rem(n, nh)
        y_copy(s, j).wait_recv()
        out_copy(yp, 1, s, j).start()
        return carry
    lax.fori_loop(0, nsub * nh, tail, 0)

    def drain(n, carry):
        s, j = n // nh, lax.rem(n, nh)
        partial_copy(s, j).wait_send()
        y_copy(s, j).wait_send()
        out_copy(yo, 0, s, j).wait()
        out_copy(yp, 1, s, j).wait()
        return carry
    lax.fori_loop(0, nsub * nh, drain, 0)
    to_far.wait_send()
    to_near.wait_send()
    pass_on.wait_send()


def solution(mesh):
    row_axes = ('dp', 'ctx')

    def device_step(hidden, w_q, w_k, w_v, w_o, k_prefix, v_prefix, k_suffix, v_suffix, seq_lens):
        nseq, model = hidden.shape
        npos, kvh, hd = k_prefix.shape
        slots = k_suffix.shape[1]
        heads = w_q.shape[1] // hd
        rows = slots * kvh
        nsub, nh = nseq // SUB, model // 2 // CB
        dims = (nseq, model, heads, kvh, hd, slots)
        hbm = pl.BlockSpec(memory_space=pl.ANY)
        dma = pltpu.SemaphoreType.DMA
        return pl.pallas_call(
            functools.partial(body, dims),
            out_shape=jax.ShapeDtypeStruct((nseq, model), BF16),
            in_specs=[hbm] * 9 + [pl.BlockSpec(memory_space=pltpu.SMEM)],
            out_specs=hbm,
            scratch_shapes=[
                pltpu.VMEM((nseq, model), BF16),
                pltpu.VMEM((nseq, model // 2), BF16),
                pltpu.VMEM((2 * nh, heads * hd, CB), BF16),
                pltpu.VMEM((RING, GRP * rows, hd), BF16),
                pltpu.VMEM((RING, GRP * rows, hd), BF16),
                pltpu.VMEM((nseq * PAD, hd), F32),
                pltpu.VMEM((heads, nseq, hd), BF16),
                pltpu.VMEM((kvh, nseq, hd), F32),
                pltpu.VMEM((kvh, nseq, hd), F32),
                pltpu.VMEM((2, npos * kvh, hd), BF16),
                pltpu.VMEM((npos * kvh, hd), F32),
                pltpu.VMEM((4, 2, kvh, npos, hd), BF16),
                pltpu.VMEM((PAD, rows), jnp.int32),
                pltpu.VMEM((SUB * PAD, hd), F32),
                pltpu.VMEM((SUB * PAD, hd), F32),
                pltpu.VMEM((SUB * PAD, hd), F32),
                pltpu.VMEM((heads, SUB, hd), BF16),
                pltpu.VMEM((nsub, nh, SUB, CB), F32),
                pltpu.VMEM((nsub, nh, SUB, CB), F32),
                pltpu.VMEM((nsub, nh, SUB, CB), F32),
                pltpu.VMEM((nsub, nh, SUB, CB), BF16),
                pltpu.VMEM((nsub, nh, SUB, CB), BF16),
                dma((2,)), dma((2,)), dma((RING, 2)), dma((2 * nh,)), dma((RING, 2)),
                dma((3,)), dma((3,)), dma((nsub, nh)), dma((nsub, nh)), dma((nsub, nh)), dma((nsub, nh)),
                dma((2, nsub, nh)),
            ],
            compiler_params=pltpu.CompilerParams(collective_id=0, has_side_effects=True,
                                                 vmem_limit_bytes=67043328),
        )(hidden, w_q, w_k, w_v, w_o,
          k_prefix.reshape(npos * kvh, hd), v_prefix.reshape(npos * kvh, hd),
          k_suffix.reshape(nseq * rows, hd), v_suffix.reshape(nseq * rows, hd), seq_lens)

    spec_in = (P(row_axes, None), P(None, 'tp'), P(None, 'tp'), P(None, 'tp'), P('tp', None), P(row_axes, 'tp', None), P(row_axes, 'tp', None), P(row_axes, None, 'tp', None), P(row_axes, None, 'tp', None), P(row_axes))
    return jax.shard_map(device_step, mesh=mesh, in_specs=spec_in, out_specs=P(row_axes, None), check_vma=False)
```

```python
import functools

import jax
import jax.numpy as jnp
from jax import lax
from jax.experimental import pallas as pl
from jax.experimental.pallas import tpu as pltpu
from jax.sharding import PartitionSpec as P

MESH = pl.DeviceIdType.MESH
F32 = jnp.float32
BF16 = jnp.bfloat16
LOG2E = 1.4426950408889634
LOW = -3.0e38

CB = 256
SUB = 32
GRP = 8
RING = 4
AHEAD = 4
WSLOT = 5
PAD = 24


def mm(a, b):
    return jnp.dot(a, b, preferred_element_type=F32)


def mmt(a, b):
    return lax.dot_general(a, b, (((1,), (1,)), ((), ())), preferred_element_type=F32)


def body(dims, hid, wq, wk, wv, wo, kp, vp, ks, vs, lens, out,
         x_v, w_v, wo_v, k_ring, v_ring, q2, qg, qs, kvn, kvs, dei, kvp, key,
         o2, m2, l2, att, snd, rcv, own, ybuf,
         x_sem, p_sem, w_sem, wo_sem, kv_sem, g_snd, g_rcv, q_snd, q_rcv, a_snd, a_rcv,
         f_snd, f_rcv, y_snd, y_rcv):
    nseq, model, heads, kvh, hd, slots = dims
    grp_heads = heads // kvh
    rows = slots * kvh
    half = model // 2
    quart = half // 2
    nq = heads * hd // 2 // CB
    nw = nq + 2
    nh = quart // CB
    nsub = nseq // SUB
    ngrp = nseq // GRP
    gps = SUB // GRP
    npos = kvp.shape[3]
    c = lax.axis_index('ctx')
    t = lax.axis_index('tp')
    core = lax.rem(c, 2)
    sib = c + 1 - 2 * core
    far = {'ctx': lax.rem(c + 2, 4)}
    near = {'ctx': sib}
    mate = {'tp': 1 - t}
    diag = {'tp': 1 - t, 'ctx': sib}
    cs = LOG2E * hd ** -0.5

    def remote(src, dst, ss, rs, dev):
        return pltpu.make_async_remote_copy(src_ref=src, dst_ref=dst, send_sem=ss, recv_sem=rs,
                                            device_id=dev, device_id_type=MESH)

    def w_copy(n):
        if n < nq:
            src, col = wq, core * (nq * CB) + n * CB
        else:
            src, col = (wk, wv)[n - nq], core * CB
        return pltpu.make_async_copy(src.at[:, pl.ds(pl.multiple_of(col, CB), CB)], w_v.at[n % WSLOT], w_sem.at[n])

    def wo_copy(j):
        side = (1 - t) if j < nh else t
        col = side * half + core * quart + (j % nh) * CB
        return pltpu.make_async_copy(wo.at[:, pl.ds(pl.multiple_of(col, CB), CB)],
                                     wo_v.at[j // 2, :, pl.ds(j % 2 * CB, CB)], wo_sem.at[j])

    def kv_copies(g):
        slot = lax.rem(g, RING)
        src = pl.ds(g * GRP * rows, GRP * rows)
        return [pltpu.make_async_copy(ks.at[src], k_ring.at[slot], kv_sem.at[slot, 0]),
                pltpu.make_async_copy(vs.at[src], v_ring.at[slot], kv_sem.at[slot, 1])]

    def kv_start(g):
        for cp in kv_copies(g):
            cp.start()

    pre = [k_ring.at[RING - 1, pl.ds(0, npos * kvh)], v_ring.at[RING - 1, pl.ds(0, npos * kvh)]]
    x_copy = pltpu.make_async_copy(hid, x_v.at[pl.ds(0, nseq)], x_sem.at[0])
    p_copies = [pltpu.make_async_copy(kp, pre[0], p_sem.at[0]), pltpu.make_async_copy(vp, pre[1], p_sem.at[1])]

    barrier = pltpu.get_barrier_semaphore()
    for dev in (near, far, mate, diag):
        pl.semaphore_signal(barrier, inc=1, device_id=dev, device_id_type=MESH)
    p_copies[0].start()
    p_copies[1].start()
    x_copy.start()
    for n in range(AHEAD):
        w_copy(n).start()

    row_head = lax.broadcasted_iota(jnp.int32, (PAD, rows), 0) // grp_heads
    col_row = lax.broadcasted_iota(jnp.int32, (PAD, rows), 1)
    key[...] = jnp.where(lax.rem(col_row, kvh) == row_head, col_row // kvh, slots)
    for h in range(heads, PAD):
        q2[pl.ds(h, nseq, stride=PAD), :] = jnp.zeros((nseq, hd), F32)

    pl.semaphore_wait(barrier, 4)
    x_send = remote(hid, x_v.at[pl.ds(nseq, nseq)], x_sem.at[1], x_sem.at[2], near)
    x_send.start()
    for i in range(2):
        p_copies[i].wait()
        dei[...] = pre[i][...].astype(F32)
        for h in range(kvh):
            kvp[0, i, h] = dei[pl.ds(h, npos, stride=kvh), :].astype(BF16)
    to_far = remote(kvp.at[0], kvp.at[2], g_snd.at[0], g_rcv.at[0], far)
    to_near = remote(kvp.at[0], kvp.at[1], g_snd.at[1], g_rcv.at[1], near)
    pass_on = remote(kvp.at[2], kvp.at[3], g_snd.at[2], g_rcv.at[2], near)
    to_far.start()

    hpb = CB // hd
    mine = core * (nq * hpb)
    theirs = (1 - core) * (nq * hpb)

    def q_copy(n):
        at = pl.ds(hpb * n, hpb)
        return remote(qs.at[at], qg.at[pl.ds(mine + hpb * n, hpb)], q_snd.at[n], q_rcv.at[n], near)

    def kv_new_copy(i):
        return remote(kvs.at[i], kvn.at[i, pl.ds(core * hpb, hpb)], q_snd.at[nq + i], q_rcv.at[nq + i], near)

    x_copy.wait()
    x_send.wait_recv()
    for n in range(nw):
        w_copy(n).wait()
        r = mm(x_v[...], w_v[n % WSLOT]).astype(BF16)
        for i in range(hpb):
            one = r[:nseq, i * hd:(i + 1) * hd]
            other = r[nseq:, i * hd:(i + 1) * hd]
            if n < nq:
                h = mine + hpb * n + i
                qg[h] = one
                q2[pl.ds(h, nseq, stride=PAD), :] = one.astype(F32)
                qs[hpb * n + i] = other
            else:
                kvn[n - nq, core * hpb + i] = one
                kvs[n - nq, i] = other
        if n < nq:
            q_copy(n).start()
        else:
            kv_new_copy(n - nq).start()
        if n + AHEAD < nw:
            w_copy(n + AHEAD).start()
        else:
            kv_start(n + AHEAD - nw)
    to_near.start()
    for n in range(nq):
        q_copy(n).wait_recv()
        for i in range(hpb):
            h = theirs + hpb * n + i
            q2[pl.ds(h, nseq, stride=PAD), :] = qg[h].astype(F32)

    zero8 = jnp.zeros((8, hd), F32)
    zero32 = jnp.zeros((32, hd), BF16)
    quarter = rows // 4

    def scores(slot, b, base):
        q = q2[pl.ds(pl.multiple_of(b * PAD, 8), PAD), :]
        q = jnp.concatenate([q, zero8], 0).astype(BF16)
        lhs = jnp.concatenate([jnp.concatenate([q, zero32], 1), jnp.concatenate([zero32, q], 1)], 0)
        s = []
        for p in range(2):
            k0 = k_ring[slot, base + 2 * p * quarter:base + (2 * p + 1) * quarter, :]
            k1 = k_ring[slot, base + (2 * p + 1) * quarter:base + (2 * p + 2) * quarter, :]
            r = mmt(lhs, jnp.concatenate([k0, k1], 1))
            s += [r[0:PAD], r[32:32 + PAD]]
        return s

    def weights(s, b):
        n_old = lens[b]
        s = [jnp.where(key[:, p * quarter:(p + 1) * quarter] < n_old, s[p], -jnp.inf) for p in range(4)]
        m = jnp.maximum(jnp.maximum(s[0], s[1]), jnp.maximum(s[2], s[3]))
        m = jnp.maximum(jnp.max(m, axis=1, keepdims=True), LOW)
        e = [jnp.exp2((a - m) * cs) for a in s]
        l = jnp.sum((e[0] + e[1]) + (e[2] + e[3]), axis=1, keepdims=True)
        gap = jnp.zeros((8, 2 * quarter), F32)
        w = jnp.concatenate([jnp.concatenate([e[0], e[2]], 1), gap,
                             jnp.concatenate([e[1], e[3]], 1), gap], 0).astype(BF16)
        at = pl.ds(pl.multiple_of(lax.rem(b, SUB) * PAD, 8), PAD)
        m2[at, :] = jnp.broadcast_to(m, (PAD, hd))
        l2[at, :] = jnp.broadcast_to(l, (PAD, hd))
        return w

    def values(w, slot, b, base):
        v = [v_ring[slot, base + p * quarter:base + (p + 1) * quarter, :] for p in range(4)]
        v = jnp.concatenate([jnp.concatenate([v[0], v[1]], 1), jnp.concatenate([v[2], v[3]], 1)], 0)
        o = mm(w, v)
        at = pl.ds(pl.multiple_of(lax.rem(b, SUB) * PAD, 8), PAD)
        o2[at, :] = o[0:PAD, :hd] + o[32:32 + PAD, hd:]

    def attend(g):
        slot = lax.rem(g, RING)
        s, w = {}, {}
        for n in range(GRP + 2):
            if n < GRP:
                s[n] = scores(slot, g * GRP + n, n * rows)
            if 0 <= n - 2 < GRP:
                values(w.pop(n - 2), slot, g * GRP + n - 2, (n - 2) * rows)
            if 0 <= n - 1 < GRP:
                w[n - 1] = weights(s.pop(n - 1), g * GRP + n - 1)

    def group(g, carry):
        for cp in kv_copies(g):
            cp.wait()
        attend(g)

        @pl.when(jnp.logical_and(g >= gps, g + RING < ngrp))
        def _():
            kv_start(g + RING)

        steps = [((0, 4), ()), ((4, 7), (0,)), ((7, 2 * nh), (1,)), ((), (2, 3))]
        for n, (wo_part, kv_part) in enumerate(steps):
            @pl.when(g == n)
            def _():
                for j in range(*wo_part) if wo_part else ():
                    wo_copy(j).start()
                for m in kv_part:
                    kv_start(RING + m)

        @pl.when(g == 1)
        def _():
            to_far.wait_recv()
            pass_on.start()
        return carry

    def merge(s):
        at = pl.ds(pl.multiple_of(s * SUB, SUB), SUB)

        def pre_scores(h):
            q = qg[h * grp_heads:(h + 1) * grp_heads, at, :].reshape(grp_heads * SUB, hd)
            return q, [mmt(q, kvp[n, 0, h]) for n in range(4)]

        def pre_weights(sc):
            m = jnp.maximum(jnp.maximum(sc[0], sc[1]), jnp.maximum(sc[2], sc[3]))
            m = jnp.max(m, axis=1, keepdims=True)
            e = [jnp.exp2((a - m) * cs) for a in sc]
            l = jnp.sum((e[0] + e[1]) + (e[2] + e[3]), axis=1, keepdims=True)
            return jnp.concatenate([a.astype(BF16) for a in e], 1), m, l

        def join(h, q, w, m, l):
            o = mm(w, jnp.concatenate([kvp[n, 1, h] for n in range(4)], 0))
            k_new = kvn[0, h, at, :].astype(F32)
            v_new = kvn[1, h, at, :].astype(F32)
            for i in range(grp_heads):
                part = slice(i * SUB, (i + 1) * SUB)
                rows_at = pl.ds(h * grp_heads + i, SUB, stride=PAD)
                m_s, l_s, o_s = m2[rows_at, :], l2[rows_at, :], o2[rows_at, :]
                s_n = jnp.sum(q[part].astype(F32) * k_new, axis=1, keepdims=True)
                m_p = jnp.maximum(m[part], s_n)
                m_all = jnp.maximum(m_p, m_s)
                w_p = jnp.exp2((m[part] - m_all) * cs)
                w_n = jnp.exp2((s_n - m_all) * cs)
                w_s = jnp.exp2((m_s - m_all) * cs)
                total = w_p * l[part] + w_n + w_s * l_s
                val = (w_p * o[part] + w_n * v_new + w_s * o_s) / total
                att[s, h * grp_heads + i, :SUB] = val.astype(BF16)

        sc, w = {}, {}
        for n in range(kvh + 2):
            if n < kvh:
                sc[n] = pre_scores(n)
            if 0 <= n - 2 < kvh:
                join(n - 2, *w.pop(n - 2))
            if 0 <= n - 1 < kvh:
                q, p = sc.pop(n - 1)
                w[n - 1] = (q,) + pre_weights(p)

    def att_copy(s):
        return remote(att.at[s, :, pl.ds(0, SUB)], att.at[s, :, pl.ds(SUB, SUB)], a_snd.at[s], a_rcv.at[s], near)

    def partial_copy(s, j):
        return remote(snd.at[s, j], rcv.at[s, j], f_snd.at[s, j], f_rcv.at[s, j], mate)

    def sub_rows(s):
        return pl.ds(pl.multiple_of(s * SUB, SUB), SUB)

    def y_col(j):
        return pl.ds(pl.multiple_of(t * half + core * quart + j * CB, CB), CB)

    def y_copies(s, j):
        there = out.at[sub_rows(s), y_col(j)]
        one, other = ybuf.at[s, j, pl.ds(0, SUB)], ybuf.at[s, j, pl.ds(SUB, SUB)]
        return [remote(one, there, y_snd.at[0, s, j], y_rcv.at[0, s, j], mate),
                remote(other, there, y_snd.at[1, s, j], y_rcv.at[1, s, j], diag),
                remote(other, there, y_snd.at[2, s, j], y_rcv.at[2, s, j], near)]

    def finish(s):
        def step(j, carry):
            partial_copy(s, j).wait_recv()
            y = (own[s, j] + rcv[s, j]).astype(BF16)
            ybuf[s, j] = y
            for cp in y_copies(s, j):
                cp.start()
            out[sub_rows(s), y_col(j)] = y[:SUB]
            return carry
        lax.fori_loop(0, nh, step, 0)

    def sub_pass(s, carry):
        lax.fori_loop(s * gps, (s + 1) * gps, group, 0)

        @pl.when(s == 0)
        def _():
            to_near.wait_recv()
            for i in range(2):
                kv_new_copy(i).wait_recv()
            pass_on.wait_recv()

        merge(s)
        att_copy(s).start()

        @pl.when(s > 0)
        def _():
            finish(s - 1)
        att_copy(s).wait_recv()

        def wo_wait(j):
            @pl.when(s == 0)
            def _():
                wo_copy(2 * j).wait()
                wo_copy(2 * j + 1).wait()

        def keep(j, p):
            x_at = jnp.concatenate([x_v[sub_rows(s), y_col(j)],
                                    x_v[pl.ds(pl.multiple_of(nseq + s * SUB, SUB), SUB), y_col(j)]], 0)
            own[s, j] = p + x_at.astype(F32)

        a = jnp.concatenate([att[s, h] for h in range(heads)], 1)
        for j in range(nh):
            wo_wait(j)
            p = mm(a, wo_v[j])
            for i in range(2):
                n = 2 * j + i
                if n < nh:
                    snd[s, n] = p[:, i * CB:(i + 1) * CB]
                    partial_copy(s, n).start()
                else:
                    keep(n - nh, p[:, i * CB:(i + 1) * CB])
        return carry

    lax.fori_loop(0, nsub, sub_pass, 0)
    finish(nsub - 1)

    def drain(n, carry):
        s, j = n // nh, lax.rem(n, nh)
        partial_copy(s, j).wait_send()
        for cp in y_copies(s, j):
            cp.wait()
        return carry
    lax.fori_loop(0, nsub * nh, drain, 0)
    for s in range(nsub):
        att_copy(s).wait_send()
    for n in range(nq):
        q_copy(n).wait_send()
    for i in range(2):
        kv_new_copy(i).wait_send()
    x_send.wait_send()
    to_far.wait_send()
    to_near.wait_send()
    pass_on.wait_send()


def solution(mesh):
    row_axes = ('dp', 'ctx')

    def device_step(hidden, w_q, w_k, w_v, w_o, k_prefix, v_prefix, k_suffix, v_suffix, seq_lens):
        nseq, model = hidden.shape
        npos, kvh, hd = k_prefix.shape
        slots = k_suffix.shape[1]
        heads = w_q.shape[1] // hd
        rows = slots * kvh
        nsub, nh = nseq // SUB, model // 4 // CB
        nw = heads * hd // 2 // CB + 2
        hpb = CB // hd
        dims = (nseq, model, heads, kvh, hd, slots)
        hbm = pl.BlockSpec(memory_space=pl.ANY)
        dma = pltpu.SemaphoreType.DMA
        return pl.pallas_call(
            functools.partial(body, dims),
            out_shape=jax.ShapeDtypeStruct((nseq, model), BF16),
            in_specs=[hbm] * 9 + [pl.BlockSpec(memory_space=pltpu.SMEM)],
            out_specs=pl.BlockSpec(memory_space=pltpu.VMEM),
            scratch_shapes=[
                pltpu.VMEM((2 * nseq, model), BF16),
                pltpu.VMEM((WSLOT, model, CB), BF16),
                pltpu.VMEM((nh, heads * hd, 2 * CB), BF16),
                pltpu.VMEM((RING, GRP * rows, hd), BF16),
                pltpu.VMEM((RING, GRP * rows, hd), BF16),
                pltpu.VMEM((nseq * PAD, hd), F32),
                pltpu.VMEM((heads, nseq, hd), BF16),
                pltpu.VMEM((heads // 2, nseq, hd), BF16),
                pltpu.VMEM((2, kvh, nseq, hd), BF16),
                pltpu.VMEM((2, hpb, nseq, hd), BF16),
                pltpu.VMEM((npos * kvh, hd), F32),
                pltpu.VMEM((4, 2, kvh, npos, hd), BF16),
                pltpu.VMEM((PAD, rows), jnp.int32),
                pltpu.VMEM((SUB * PAD, hd), F32),
                pltpu.VMEM((SUB * PAD, hd), F32),
                pltpu.VMEM((SUB * PAD, hd), F32),
                pltpu.VMEM((nsub, heads, 2 * SUB, hd), BF16),
                pltpu.VMEM((nsub, nh, 2 * SUB, CB), F32),
                pltpu.VMEM((nsub, nh, 2 * SUB, CB), F32),
                pltpu.VMEM((nsub, nh, 2 * SUB, CB), F32),
                pltpu.VMEM((nsub, nh, 2 * SUB, CB), BF16),
                dma((3,)), dma((2,)), dma((nw,)), dma((2 * nh,)), dma((RING, 2)),
                dma((3,)), dma((3,)), dma((nw,)), dma((nw,)), dma((nsub,)), dma((nsub,)),
                dma((nsub, nh)), dma((nsub, nh)), dma((3, nsub, nh)), dma((3, nsub, nh)),
            ],
            compiler_params=pltpu.CompilerParams(collective_id=0, has_side_effects=True,
                                                 vmem_limit_bytes=67043328),
        )(hidden, w_q, w_k, w_v, w_o,
          k_prefix.reshape(npos * kvh, hd), v_prefix.reshape(npos * kvh, hd),
          k_suffix.reshape(nseq * rows, hd), v_suffix.reshape(nseq * rows, hd), seq_lens)

    spec_in = (P(row_axes, None), P(None, 'tp'), P(None, 'tp'), P(None, 'tp'), P('tp', None), P(row_axes, 'tp', None), P(row_axes, 'tp', None), P(row_axes, None, 'tp', None), P(row_axes, None, 'tp', None), P(row_axes))
    return jax.shard_map(device_step, mesh=mesh, in_specs=spec_in, out_specs=P(row_axes, None), check_vma=False)
```

```python
import functools

import jax
import jax.numpy as jnp
from jax import lax
from jax.experimental import pallas as pl
from jax.experimental.pallas import tpu as pltpu
from jax.sharding import PartitionSpec as P

MESH = pl.DeviceIdType.MESH
F32 = jnp.float32
BF16 = jnp.bfloat16
LOG2E = 1.4426950408889634
LOW = -3.0e38

CB = 256
PASSES = (32, 32, 32, 32)
GRP = 8
RING = 4
AHEAD = 4
PAD = 24


def mm(a, b):
    return jnp.dot(a, b, preferred_element_type=F32)


def mmt(a, b):
    return lax.dot_general(a, b, (((1,), (1,)), ((), ())), preferred_element_type=F32)


def body(dims, hid, wq, wk, wv, wo, kp, vp, ks, vs, lens, out,
         x_v, w_v, wo_v, k_ring, v_ring, q2, qg, qs, kvn, kvs, kvp, key,
         o2, m2, att, snd, rcv, own, ybuf,
         x_sem, p_sem, n_sem, w_sem, wo_sem, kv_sem, g_snd, g_rcv, q_snd, q_rcv, a_snd, a_rcv,
         f_snd, f_rcv, y_snd, y_rcv):
    nseq, model, heads, kvh, hd, slots = dims
    grp_heads = heads // kvh
    rows = slots * kvh
    half = model // 2
    quart = half // 2
    nq = heads * hd // 2 // CB
    nw = nq + 2
    nh = quart // CB
    ngrp = nseq // GRP
    starts = [sum(PASSES[:p]) for p in range(len(PASSES))]
    npos = kvp.shape[3]
    c = lax.axis_index('ctx')
    t = lax.axis_index('tp')
    core = lax.rem(c, 2)
    sib = c + 1 - 2 * core
    far = {'ctx': lax.rem(c + 2, 4)}
    near = {'ctx': sib}
    mate = {'tp': 1 - t}
    diag = {'tp': 1 - t, 'ctx': sib}
    cs = LOG2E * hd ** -0.5

    def remote(src, dst, ss, rs, dev):
        return pltpu.make_async_remote_copy(src_ref=src, dst_ref=dst, send_sem=ss, recv_sem=rs,
                                            device_id=dev, device_id_type=MESH)

    def w_copy(n):
        if n < nq:
            src, col = wq, core * (nq * CB) + n * CB
        else:
            src, col = (wk, wv)[n - nq], core * CB
        return pltpu.make_async_copy(src.at[:, pl.ds(pl.multiple_of(col, CB), CB)], w_v.at[n], w_sem.at[n])

    def wo_copy(j):
        side = (1 - t) if j < nh else t
        col = side * half + core * quart + (j % nh) * CB
        return pltpu.make_async_copy(wo.at[:, pl.ds(pl.multiple_of(col, CB), CB)],
                                     wo_v.at[j // 2, :, pl.ds(j % 2 * CB, CB)], wo_sem.at[j])

    def kv_copies(g):
        slot = lax.rem(g, RING)
        src = pl.ds(g * GRP * rows, GRP * rows)
        return [pltpu.make_async_copy(ks.at[src], k_ring.at[slot], kv_sem.at[slot, 0]),
                pltpu.make_async_copy(vs.at[src], v_ring.at[slot], kv_sem.at[slot, 1])]

    def kv_start(g):
        for cp in kv_copies(g):
            cp.start()

    pre = [k_ring.at[RING - 1, pl.ds(0, npos * kvh)], v_ring.at[RING - 1, pl.ds(0, npos * kvh)]]
    x_copy = pltpu.make_async_copy(hid, x_v.at[pl.ds(0, nseq)], x_sem.at[0])
    p_copies = [pltpu.make_async_copy(kp, pre[0], p_sem.at[0]), pltpu.make_async_copy(vp, pre[1], p_sem.at[1])]

    barrier = pltpu.get_barrier_semaphore()
    for dev in (near, far, mate, diag):
        pl.semaphore_signal(barrier, inc=1, device_id=dev, device_id_type=MESH)
    p_copies[0].start()
    p_copies[1].start()
    x_copy.start()
    for n in range(AHEAD):
        w_copy(n).start()

    dei = q2.at[pl.ds(0, npos * kvh)]
    for i in range(2):
        p_copies[i].wait()
        dei[...] = pre[i][...].astype(F32)
        for h in range(kvh):
            kvp[0, h, i] = dei[pl.ds(h, npos, stride=kvh), :].astype(BF16)
    to_far = [remote(kvp.at[0, h], kvp.at[2, h], g_snd.at[0, h], g_rcv.at[0, h], far) for h in range(kvh)]
    pass_on = [remote(kvp.at[2, h], kvp.at[3, h], g_snd.at[1, h], g_rcv.at[1, h], near) for h in range(kvh)]
    to_near = remote(kvp.at[0], kvp.at[1], n_sem.at[0], n_sem.at[1], near)
    x_send = remote(x_v.at[pl.ds(0, nseq)], x_v.at[pl.ds(nseq, nseq)], x_sem.at[1], x_sem.at[2], near)
    x_copy.wait()
    pl.semaphore_wait(barrier, 4)
    for cp in to_far:
        cp.start()
    x_send.start()

    row_head = lax.broadcasted_iota(jnp.int32, (PAD, rows), 0) // grp_heads
    col_row = lax.broadcasted_iota(jnp.int32, (PAD, rows), 1)
    key[...] = jnp.where(lax.rem(col_row, kvh) == row_head, col_row // kvh, slots)
    for h in range(heads, PAD):
        q2[pl.ds(h, nseq, stride=PAD), :] = jnp.zeros((nseq, hd), F32)

    hpb = CB // hd
    mine = core * (nq * hpb)
    theirs = (1 - core) * (nq * hpb)

    def q_copy(n):
        at = pl.ds(hpb * n, hpb)
        return remote(qs.at[at], qg.at[pl.ds(mine + hpb * n, hpb)], q_snd.at[n], q_rcv.at[n], near)

    def kv_new_copy(i):
        return remote(kvs.at[i], kvn.at[i, pl.ds(core * hpb, hpb)], q_snd.at[nq + i], q_rcv.at[nq + i], near)

    def rows_dot(lo, n):
        r = [mm(x_v[lo + i * (nseq // 2):lo + (i + 1) * (nseq // 2)], w_v[n]) for i in range(2)]
        return jnp.concatenate(r, 0).astype(BF16)

    for n in range(nw):
        w_copy(n).wait()
        r = rows_dot(0, n)
        for i in range(hpb):
            one = r[:, i * hd:(i + 1) * hd]
            if n < nq:
                h = mine + hpb * n + i
                qg[h] = one
                q2[pl.ds(h, nseq, stride=PAD), :] = one.astype(F32)
            else:
                kvn[n - nq, core * hpb + i] = one
        if n + AHEAD < nw:
            w_copy(n + AHEAD).start()
        else:
            kv_start(n + AHEAD - nw)
    x_send.wait_recv()
    for n in range(nw):
        r = rows_dot(nseq, n)
        for i in range(hpb):
            one = r[:, i * hd:(i + 1) * hd]
            if n < nq:
                qs[hpb * n + i] = one
            else:
                kvs[n - nq, i] = one
        if n < nq:
            q_copy(n).start()
        else:
            kv_new_copy(n - nq).start()
    to_near.start()
    for n in range(nq):
        q_copy(n).wait_recv()
        for i in range(hpb):
            h = theirs + hpb * n + i
            q2[pl.ds(h, nseq, stride=PAD), :] = qg[h].astype(F32)

    zero8 = jnp.zeros((8, hd), F32)
    zero32 = jnp.zeros((32, hd), BF16)
    quarter = rows // 4

    def scores(slot, b, base):
        q = q2[pl.ds(pl.multiple_of(b * PAD, 8), PAD), :]
        q = jnp.concatenate([q, zero8], 0).astype(BF16)
        lhs = jnp.concatenate([jnp.concatenate([q, zero32], 1), jnp.concatenate([zero32, q], 1)], 0)
        s = []
        for p in range(2):
            k0 = k_ring[slot, base + 2 * p * quarter:base + (2 * p + 1) * quarter, :]
            k1 = k_ring[slot, base + (2 * p + 1) * quarter:base + (2 * p + 2) * quarter, :]
            r = mmt(lhs, jnp.concatenate([k0, k1], 1))
            s += [r[0:PAD], r[32:32 + PAD]]
        return s

    def weights(s, b):
        n_old = lens[b]
        s = [jnp.where(key[:, p * quarter:(p + 1) * quarter] < n_old, s[p], -jnp.inf) for p in range(4)]
        m = jnp.maximum(jnp.maximum(s[0], s[1]), jnp.maximum(s[2], s[3]))
        m = jnp.maximum(jnp.max(m, axis=1, keepdims=True), LOW)
        e = [jnp.exp2((a - m) * cs) for a in s]
        l = jnp.sum((e[0] + e[1]) + (e[2] + e[3]), axis=1, keepdims=True)
        gap = jnp.zeros((8, 2 * quarter), F32)
        w = jnp.concatenate([jnp.concatenate([e[0], e[2]], 1), gap,
                             jnp.concatenate([e[1], e[3]], 1), gap], 0).astype(BF16)
        return w, m, l

    def values(w, m, l, slot, base, local):
        v = [v_ring[slot, base + p * quarter:base + (p + 1) * quarter, :] for p in range(4)]
        v = jnp.concatenate([jnp.concatenate([v[0], v[1]], 1), jnp.concatenate([v[2], v[3]], 1)], 0)
        o = mm(w, v)
        at = pl.ds(pl.multiple_of(local * PAD, 8), PAD)
        o2[at, :] = (o[0:PAD, :hd] + o[32:32 + PAD, hd:]) / jnp.maximum(l, 1.0)
        m2[at, :] = jnp.broadcast_to(m + jnp.log2(l) / cs, (PAD, hd))

    per = 2 * GRP

    def attend(d, first):
        for i in range(2):
            for cp in kv_copies(2 * d + i):
                cp.wait()
        slots_of = [lax.rem(2 * d + i, RING) for i in range(2)]
        s, w = {}, {}
        for n in range(per + 2):
            if n < per:
                s[n] = scores(slots_of[n // GRP], d * per + n, n % GRP * rows)
            if 0 <= n - 2 < per:
                m = n - 2
                values(*w.pop(m), slots_of[m // GRP], m % GRP * rows, d * per + m - first)
            if 0 <= n - 1 < per:
                w[n - 1] = weights(s.pop(n - 1), d * per + n - 1)

    def refill(d):
        for i in range(2):
            kv_start(2 * d + RING + i)

    def merge(p, before):
        size, lo = PASSES[p], starts[p]
        at = pl.ds(lo, size)

        def pre_scores(h):
            q = qg[h * grp_heads:(h + 1) * grp_heads, at, :].reshape(grp_heads * size, hd)
            return q, [mmt(q, kvp[n, h, 0]) for n in range(4)]

        def pre_weights(sc):
            m = jnp.maximum(jnp.maximum(sc[0], sc[1]), jnp.maximum(sc[2], sc[3]))
            m = jnp.max(m, axis=1, keepdims=True)
            e = [jnp.exp2((a - m) * cs) for a in sc]
            l = jnp.sum((e[0] + e[1]) + (e[2] + e[3]), axis=1, keepdims=True)
            return jnp.concatenate([a.astype(BF16) for a in e], 1), m, l

        def join(h, q, w, m, l):
            o = mm(w, jnp.concatenate([kvp[n, h, 1] for n in range(4)], 0))
            k_new = kvn[0, h, at, :].astype(F32)
            v_new = kvn[1, h, at, :].astype(F32)
            for i in range(grp_heads):
                part = slice(i * size, (i + 1) * size)
                rows_at = pl.ds(h * grp_heads + i, size, stride=PAD)
                m_s, o_s = m2[rows_at, :], o2[rows_at, :]
                s_n = jnp.sum(q[part].astype(F32) * k_new, axis=1, keepdims=True)
                m_p = jnp.maximum(m[part], s_n)
                m_all = jnp.maximum(m_p, m_s)
                w_p = jnp.exp2((m[part] - m_all) * cs)
                w_n = jnp.exp2((s_n - m_all) * cs)
                w_s = jnp.exp2((m_s - m_all) * cs)
                total = w_p * l[part] + w_n + w_s
                val = (w_p * o[part] + w_n * v_new + w_s * o_s) / total
                att[h * grp_heads + i, 2 * lo:2 * lo + size] = val.astype(BF16)

        sc, w = {}, {}
        for n in range(kvh + 2):
            if n < kvh:
                before(n)
                sc[n] = pre_scores(n)
            if 0 <= n - 2 < kvh:
                join(n - 2, *w.pop(n - 2))
                att_copy(p, n - 2).start()
            if 0 <= n - 1 < kvh:
                q, part = sc.pop(n - 1)
                w[n - 1] = (q,) + pre_weights(part)

    def att_copy(p, h):
        heads_at = pl.ds(h * grp_heads, grp_heads)
        lo, size = 2 * starts[p], PASSES[p]
        return remote(att.at[heads_at, pl.ds(lo, size)], att.at[heads_at, pl.ds(lo + size, size)],
                      a_snd.at[p, h], a_rcv.at[p, h], near)

    def both(p):
        return pl.ds(2 * starts[p], 2 * PASSES[p])

    def partial_copy(p, j):
        return remote(snd.at[j, both(p)], rcv.at[j, both(p)], f_snd.at[p, j], f_rcv.at[p, j], mate)

    def y_col(j):
        return pl.ds(pl.multiple_of(t * half + core * quart + j * CB, CB), CB)

    def y_copies(p, j):
        size = PASSES[p]
        there = out.at[pl.ds(starts[p], size), y_col(j)]
        one, other = [ybuf.at[j, pl.ds(2 * starts[p] + i * size, size)] for i in range(2)]
        return [remote(one, there, y_snd.at[0, p, j], y_rcv.at[0, p, j], mate),
                remote(other, there, y_snd.at[1, p, j], y_rcv.at[1, p, j], diag),
                remote(other, there, y_snd.at[2, p, j], y_rcv.at[2, p, j], near)]

    def finish(p):
        for j in range(nh):
            partial_copy(p, j).wait_recv()
            y = (own[j, both(p)] + rcv[j, both(p)]).astype(BF16)
            ybuf[j, both(p)] = y
            for cp in y_copies(p, j):
                cp.start()
            out[pl.ds(starts[p], PASSES[p]), y_col(j)] = y[:PASSES[p]]

    def project(p):
        size, lo = PASSES[p], starts[p]
        for h in range(kvh):
            att_copy(p, h).wait_recv()
        a = jnp.concatenate([att[h, both(p)] for h in range(heads)], 1)
        for j in range(nh):
            if p == 0:
                wo_copy(2 * j).wait()
                wo_copy(2 * j + 1).wait()
            r = mm(a, wo_v[j])
            for i in range(2):
                n = 2 * j + i
                part = r[:, i * CB:(i + 1) * CB]
                if n < nh:
                    snd[n, both(p)] = part
                    partial_copy(p, n).start()
                else:
                    x_at = jnp.concatenate([x_v[pl.ds(lo, size), y_col(n - nh)],
                                            x_v[pl.ds(nseq + lo, size), y_col(n - nh)]], 0)
                    own[n - nh, both(p)] = part + x_at.astype(F32)

    def forward(h):
        to_far[h].wait_recv()
        pass_on[h].start()

    def need(h):
        if h == 0:
            to_near.wait_recv()
            for i in range(2):
                kv_new_copy(i).wait_recv()
        if h == 2:
            forward(kvh - 1)
        pass_on[h].wait_recv()

    npass = len(PASSES)
    for p in range(npass):
        d0, d1 = starts[p] // per, (starts[p] + PASSES[p]) // per
        if p == 0:
            forward(0)
            for d in range(d0, d1):
                attend(d, 0)
                refill(d)
                if d < 2:
                    for j in range(nh * d, nh * (d + 1)):
                        wo_copy(j).start()
                    forward(1 + d)
            merge(p, need)
        else:
            def step(d, carry):
                attend(d, starts[p])

                @pl.when(2 * d + RING < ngrp)
                def _():
                    refill(d)
                return carry
            lax.fori_loop(d0, d1, step, 0)
            merge(p, lambda h: None)
        project(p)
        if p > 0:
            finish(p - 1)
    finish(npass - 1)

    for p in range(npass):
        for j in range(nh):
            partial_copy(p, j).wait_send()
            for cp in y_copies(p, j):
                cp.wait()
        for h in range(kvh):
            att_copy(p, h).wait_send()
    for n in range(nq):
        q_copy(n).wait_send()
    for i in range(2):
        kv_new_copy(i).wait_send()
    x_send.wait_send()
    to_near.wait_send()
    for h in range(kvh):
        to_far[h].wait_send()
        pass_on[h].wait_send()


def solution(mesh):
    row_axes = ('dp', 'ctx')

    def device_step(hidden, w_q, w_k, w_v, w_o, k_prefix, v_prefix, k_suffix, v_suffix, seq_lens):
        nseq, model = hidden.shape
        npos, kvh, hd = k_prefix.shape
        slots = k_suffix.shape[1]
        heads = w_q.shape[1] // hd
        rows = slots * kvh
        npass, nh = len(PASSES), model // 4 // CB
        nw = heads * hd // 2 // CB + 2
        hpb = CB // hd
        dims = (nseq, model, heads, kvh, hd, slots)
        hbm = pl.BlockSpec(memory_space=pl.ANY)
        dma = pltpu.SemaphoreType.DMA
        return pl.pallas_call(
            functools.partial(body, dims),
            out_shape=jax.ShapeDtypeStruct((nseq, model), BF16),
            in_specs=[hbm] * 9 + [pl.BlockSpec(memory_space=pltpu.SMEM)],
            out_specs=pl.BlockSpec(memory_space=pltpu.VMEM),
            scratch_shapes=[
                pltpu.VMEM((2 * nseq, model), BF16),
                pltpu.VMEM((nw, model, CB), BF16),
                pltpu.VMEM((nh, heads * hd, 2 * CB), BF16),
                pltpu.VMEM((RING, GRP * rows, hd), BF16),
                pltpu.VMEM((RING, GRP * rows, hd), BF16),
                pltpu.VMEM((nseq * PAD, hd), F32),
                pltpu.VMEM((heads, nseq, hd), BF16),
                pltpu.VMEM((heads // 2, nseq, hd), BF16),
                pltpu.VMEM((2, kvh, nseq, hd), BF16),
                pltpu.VMEM((2, hpb, nseq, hd), BF16),
                pltpu.VMEM((4, kvh, 2, npos, hd), BF16),
                pltpu.VMEM((PAD, rows), jnp.int32),
                pltpu.VMEM((max(PASSES) * PAD, hd), F32),
                pltpu.VMEM((max(PASSES) * PAD, hd), F32),
                pltpu.VMEM((heads, 2 * nseq, hd), BF16),
                pltpu.VMEM((nh, 2 * nseq, CB), F32),
                pltpu.VMEM((nh, 2 * nseq, CB), F32),
                pltpu.VMEM((nh, 2 * nseq, CB), F32),
                pltpu.VMEM((nh, 2 * nseq, CB), BF16),
                dma((3,)), dma((2,)), dma((2,)), dma((nw,)), dma((2 * nh,)), dma((RING, 2)),
                dma((2, kvh)), dma((2, kvh)), dma((nw,)), dma((nw,)), dma((npass, kvh)), dma((npass, kvh)),
                dma((npass, nh)), dma((npass, nh)), dma((3, npass, nh)), dma((3, npass, nh)),
            ],
            compiler_params=pltpu.CompilerParams(collective_id=0, has_side_effects=True,
                                                 vmem_limit_bytes=67043328),
        )(hidden, w_q, w_k, w_v, w_o,
          k_prefix.reshape(npos * kvh, hd), v_prefix.reshape(npos * kvh, hd),
          k_suffix.reshape(nseq * rows, hd), v_suffix.reshape(nseq * rows, hd), seq_lens)

    spec_in = (P(row_axes, None), P(None, 'tp'), P(None, 'tp'), P(None, 'tp'), P('tp', None), P(row_axes, 'tp', None), P(row_axes, 'tp', None), P(row_axes, None, 'tp', None), P(row_axes, None, 'tp', None), P(row_axes))
    return jax.shard_map(device_step, mesh=mesh, in_specs=spec_in, out_specs=P(row_axes, None), check_vma=False)
```

```python
import functools

import jax
import jax.numpy as jnp
from jax import lax
from jax.experimental import pallas as pl
from jax.experimental.pallas import tpu as pltpu
from jax.sharding import PartitionSpec as P

MESH = pl.DeviceIdType.MESH
F32 = jnp.float32
BF16 = jnp.bfloat16
LOG2E = 1.4426950408889634
LOW = -3.0e38

CB = 256
SUB = 32
GRP = 8
RING = 4
AHEAD = 3
PAD = 24


def mm(a, b):
    return jnp.dot(a, b, preferred_element_type=F32)


def mmt(a, b):
    return lax.dot_general(a, b, (((1,), (1,)), ((), ())), preferred_element_type=F32)


def body(dims, hid, wq, wk, wv, wo, kp, vp, ks, vs, lens, out,
         x_v, w_v, wo_v, k_ring, v_ring, q2, qg, qs, kvn, kvs, kvp, key,
         o2, m2, snd, rcv, own,
         x_sem, p_sem, n_sem, w_sem, wo_sem, kv_sem, g_snd, g_rcv, q_snd, q_rcv, a_snd, a_rcv,
         f_snd, f_rcv, y_snd, y_rcv):
    nseq, model, heads, kvh, hd, slots = dims
    grp_heads = heads // kvh
    rows = slots * kvh
    half = model // 2
    quart = half // 2
    nq = heads * hd // 2 // CB
    nw = nq + 2
    nh = quart // CB
    ngrp = nseq // GRP
    npass = nseq // SUB
    npos = kvp.shape[3]
    c = lax.axis_index('ctx')
    t = lax.axis_index('tp')
    core = lax.rem(c, 2)
    sib = c + 1 - 2 * core
    far = {'ctx': lax.rem(c + 2, 4)}
    near = {'ctx': sib}
    mate = {'tp': 1 - t}
    diag = {'tp': 1 - t, 'ctx': sib}
    cs = LOG2E * hd ** -0.5

    def remote(src, dst, ss, rs, dev):
        return pltpu.make_async_remote_copy(src_ref=src, dst_ref=dst, send_sem=ss, recv_sem=rs,
                                            device_id=dev, device_id_type=MESH)

    def w_copy(n):
        if n < nq:
            src, col = wq, core * (nq * CB) + n * CB
        else:
            src, col = (wk, wv)[n - nq], core * CB
        return pltpu.make_async_copy(src.at[:, pl.ds(pl.multiple_of(col, CB), CB)], w_v.at[n], w_sem.at[n])

    def wo_copy(j):
        side = (1 - t) if j < nh else t
        col = side * half + core * quart + (j % nh) * CB
        return pltpu.make_async_copy(wo.at[:, pl.ds(pl.multiple_of(col, CB), CB)],
                                     wo_v.at[j // 2, :, pl.ds(j % 2 * CB, CB)], wo_sem.at[j])

    def kv_copies(g):
        slot = lax.rem(g, RING)
        src = pl.ds(g * GRP * rows, GRP * rows)
        return [pltpu.make_async_copy(ks.at[src], k_ring.at[slot], kv_sem.at[slot, 0]),
                pltpu.make_async_copy(vs.at[src], v_ring.at[slot], kv_sem.at[slot, 1])]

    def kv_start(g):
        for cp in kv_copies(g):
            cp.start()

    pre = [k_ring.at[RING - 1, pl.ds(0, npos * kvh)], v_ring.at[RING - 1, pl.ds(0, npos * kvh)]]
    x_copy = pltpu.make_async_copy(hid, x_v.at[pl.ds(0, nseq)], x_sem.at[0])
    p_copies = [pltpu.make_async_copy(kp, pre[0], p_sem.at[0]), pltpu.make_async_copy(vp, pre[1], p_sem.at[1])]

    barrier = pltpu.get_barrier_semaphore()
    for dev in (near, far, mate, diag):
        pl.semaphore_signal(barrier, inc=1, device_id=dev, device_id_type=MESH)
    p_copies[0].start()
    p_copies[1].start()
    x_copy.start()
    for n in range(AHEAD):
        w_copy(n).start()

    dei = q2.at[pl.ds(0, npos * kvh)]
    for i in range(2):
        p_copies[i].wait()
        dei[...] = pre[i][...].astype(F32)
        for h in range(kvh):
            kvp[0, h, i] = dei[pl.ds(h, npos, stride=kvh), :].astype(BF16)
    to_far = [remote(kvp.at[0, h], kvp.at[2, h], g_snd.at[0, h], g_rcv.at[0, h], far) for h in range(kvh)]
    pass_on = [remote(kvp.at[2, h], kvp.at[3, h], g_snd.at[1, h], g_rcv.at[1, h], near) for h in range(kvh)]
    to_near = remote(kvp.at[0], kvp.at[1], n_sem.at[0], n_sem.at[1], near)
    x_send = remote(x_v.at[pl.ds(0, nseq)], x_v.at[pl.ds(nseq, nseq)], x_sem.at[1], x_sem.at[2], near)
    x_copy.wait()
    pl.semaphore_wait(barrier, 4)
    for cp in to_far:
        cp.start()
    x_send.start()

    row_head = lax.broadcasted_iota(jnp.int32, (PAD, rows), 0) // grp_heads
    col_row = lax.broadcasted_iota(jnp.int32, (PAD, rows), 1)
    key[...] = jnp.where(lax.rem(col_row, kvh) == row_head, col_row // kvh, slots)
    for h in range(heads, PAD):
        q2[pl.ds(h, nseq, stride=PAD), :] = jnp.zeros((nseq, hd), F32)

    hpb = CB // hd
    mine = core * (nq * hpb)
    theirs = (1 - core) * (nq * hpb)

    def q_copy(n):
        at = pl.ds(hpb * n, hpb)
        return remote(qs.at[at], qg.at[pl.ds(mine + hpb * n, hpb)], q_snd.at[n], q_rcv.at[n], near)

    def kv_new_copy(i):
        return remote(kvs.at[i], kvn.at[i, pl.ds(core * hpb, hpb)], q_snd.at[nq + i], q_rcv.at[nq + i], near)

    def block_dot(lo, n):
        return mm(x_v[lo:lo + nseq], w_v[n]).astype(BF16)

    def put_own(n, r):
        for i in range(hpb):
            one = r[:, i * hd:(i + 1) * hd]
            if n < nq:
                h = mine + hpb * n + i
                qg[h] = one
                q2[pl.ds(h, nseq, stride=PAD), :] = one.astype(F32)
            else:
                kvn[n - nq, core * hpb + i] = one

    def put_other(n, r):
        for i in range(hpb):
            one = r[:, i * hd:(i + 1) * hd]
            if n < nq:
                qs[hpb * n + i] = one
            else:
                kvs[n - nq, i] = one
        if n < nq:
            q_copy(n).start()
        else:
            kv_new_copy(n - nq).start()

    todo = [(0, n) for n in range(nw)] + [(nseq, n) for n in range(nw)]
    for i in range(0, len(todo), 2):
        pair = todo[i:i + 2]
        for lo, n in pair:
            if lo == 0:
                w_copy(n).wait()
                if n + AHEAD < nw:
                    w_copy(n + AHEAD).start()
                else:
                    kv_start(n + AHEAD - nw)
            elif n == 0:
                x_send.wait_recv()
        r = [block_dot(lo, n) for lo, n in pair]
        for (lo, n), one in zip(pair, r):
            (put_other if lo else put_own)(n, one)
    kv_start(RING - 1)
    to_near.start()
    for n in range(nq):
        q_copy(n).wait_recv()
        for i in range(hpb):
            h = theirs + hpb * n + i
            q2[pl.ds(h, nseq, stride=PAD), :] = qg[h].astype(F32)

    zero8 = jnp.zeros((8, hd), F32)
    zero32 = jnp.zeros((32, hd), BF16)
    quarter = rows // 4

    def scores(slot, b, base):
        q = q2[pl.ds(pl.multiple_of(b * PAD, 8), PAD), :]
        q = jnp.concatenate([q, zero8], 0).astype(BF16)
        lhs = jnp.concatenate([jnp.concatenate([q, zero32], 1), jnp.concatenate([zero32, q], 1)], 0)
        s = []
        for p in range(2):
            k0 = k_ring[slot, base + 2 * p * quarter:base + (2 * p + 1) * quarter, :]
            k1 = k_ring[slot, base + (2 * p + 1) * quarter:base + (2 * p + 2) * quarter, :]
            r = mmt(lhs, jnp.concatenate([k0, k1], 1))
            s += [r[0:PAD], r[32:32 + PAD]]
        return s

    def weights(s, b):
        n_old = lens[b]
        s = [jnp.where(key[:, p * quarter:(p + 1) * quarter] < n_old, s[p], -jnp.inf) for p in range(4)]
        m = jnp.maximum(jnp.maximum(s[0], s[1]), jnp.maximum(s[2], s[3]))
        m = jnp.maximum(jnp.max(m, axis=1, keepdims=True), LOW)
        e = [jnp.exp2((a - m) * cs) for a in s]
        l = jnp.sum((e[0] + e[1]) + (e[2] + e[3]), axis=1, keepdims=True)
        gap = jnp.zeros((8, 2 * quarter), F32)
        w = jnp.concatenate([jnp.concatenate([e[0], e[2]], 1), gap,
                             jnp.concatenate([e[1], e[3]], 1), gap], 0).astype(BF16)
        return w, m, l

    def values(w, m, l, slot, base, local):
        v = [v_ring[slot, base + p * quarter:base + (p + 1) * quarter, :] for p in range(4)]
        v = jnp.concatenate([jnp.concatenate([v[0], v[1]], 1), jnp.concatenate([v[2], v[3]], 1)], 0)
        o = mm(w, v)
        at = pl.ds(pl.multiple_of(local * PAD, 8), PAD)
        o2[at, :] = (o[0:PAD, :hd] + o[32:32 + PAD, hd:]) / jnp.maximum(l, 1.0)
        m2[at, :] = jnp.broadcast_to(m + jnp.log2(l) / cs, (PAD, hd))

    per = 2 * GRP

    def attend(d, first):
        for i in range(2):
            for cp in kv_copies(2 * d + i):
                cp.wait()
        slots_of = [lax.rem(2 * d + i, RING) for i in range(2)]
        s, w = {}, {}
        for n in range(per + 2):
            if n < per:
                s[n] = scores(slots_of[n // GRP], d * per + n, n % GRP * rows)
            if 0 <= n - 2 < per:
                m = n - 2
                values(*w.pop(m), slots_of[m // GRP], m % GRP * rows, d * per + m - first)
            if 0 <= n - 1 < per:
                w[n - 1] = weights(s.pop(n - 1), d * per + n - 1)

    def refill(d):
        for i in range(2):
            kv_start(2 * d + RING + i)

    ybuf = w_v.at[0]

    def at_rows(lo, step, size):
        return pl.ds(lo if isinstance(lo, int) else pl.multiple_of(lo, step), size)

    def att_at(p, side, h, count):
        lo = 2 * p * SUB * heads + (side * heads + h) * SUB
        return w_v.at[1, at_rows(lo, SUB, count * SUB), pl.ds(0, hd)]

    def seqs(p):
        return at_rows(p * SUB, SUB, SUB)

    def both(p):
        return at_rows(2 * p * SUB, 2 * SUB, 2 * SUB)

    def y_rows(p, j, side, count):
        return at_rows(2 * (j * nseq + p * SUB) + side * SUB, SUB, count * SUB)

    def merge(p, some, before=lambda h: None):
        size = SUB
        at = seqs(p)

        def pre_scores(h):
            q = qg[h * grp_heads:(h + 1) * grp_heads, at, :].reshape(grp_heads * size, hd)
            return q, [mmt(q, kvp[n, h, 0]) for n in range(4)]

        def pre_weights(sc):
            m = jnp.maximum(jnp.maximum(sc[0], sc[1]), jnp.maximum(sc[2], sc[3]))
            m = jnp.max(m, axis=1, keepdims=True)
            e = [jnp.exp2((a - m) * cs) for a in sc]
            l = jnp.sum((e[0] + e[1]) + (e[2] + e[3]), axis=1, keepdims=True)
            return jnp.concatenate([a.astype(BF16) for a in e], 1), m, l

        def join(h, q, w, m, l):
            o = mm(w, jnp.concatenate([kvp[n, h, 1] for n in range(4)], 0))
            k_new = kvn[0, h, at, :].astype(F32)
            v_new = kvn[1, h, at, :].astype(F32)
            for i in range(grp_heads):
                part = slice(i * size, (i + 1) * size)
                rows_at = pl.ds(h * grp_heads + i, size, stride=PAD)
                m_s, o_s = m2[rows_at, :], o2[rows_at, :]
                s_n = jnp.sum(q[part].astype(F32) * k_new, axis=1, keepdims=True)
                m_p = jnp.maximum(m[part], s_n)
                m_all = jnp.maximum(m_p, m_s)
                w_p = jnp.exp2((m[part] - m_all) * cs)
                w_n = jnp.exp2((s_n - m_all) * cs)
                w_s = jnp.exp2((m_s - m_all) * cs)
                total = w_p * l[part] + w_n + w_s
                val = (w_p * o[part] + w_n * v_new + w_s * o_s) / total
                att_at(p, 0, h * grp_heads + i, 1)[...] = val.astype(BF16)

        sc, w = {}, {}
        for n in range(len(some) + 2):
            if n < len(some):
                before(some[n])
                sc[n] = pre_scores(some[n])
            if 0 <= n - 2:
                join(some[n - 2], *w.pop(n - 2))
                att_copy(p, some[n - 2]).start()
            if 0 <= n - 1 < len(some):
                q, part = sc.pop(n - 1)
                w[n - 1] = (q,) + pre_weights(part)

    def att_copy(p, h):
        mine_at, theirs_at = [att_at(p, side, h * grp_heads, grp_heads) for side in range(2)]
        return remote(mine_at, theirs_at, a_snd.at[p, h], a_rcv.at[p, h], near)

    def partial_copy(p, j):
        return remote(snd.at[j, both(p)], rcv.at[j, both(p)], f_snd.at[p, j], f_rcv.at[p, j], mate)

    def y_col(j):
        return pl.ds(pl.multiple_of(t * half + core * quart + j * CB, CB), CB)

    def y_copies(p, j):
        there = out.at[seqs(p), y_col(j)]
        one, other = [ybuf.at[y_rows(p, j, side, 1)] for side in range(2)]
        return [remote(one, there, y_snd.at[0, p, j], y_rcv.at[0, p, j], mate),
                remote(other, there, y_snd.at[1, p, j], y_rcv.at[1, p, j], diag),
                remote(other, there, y_snd.at[2, p, j], y_rcv.at[2, p, j], near)]

    def finish(p):
        for j in range(nh):
            partial_copy(p, j).wait_recv()
            y = (own[j, both(p)] + rcv[j, both(p)]).astype(BF16)
            ybuf[y_rows(p, j, 0, 2)] = y
            for cp in y_copies(p, j):
                cp.start()
            out[seqs(p), y_col(j)] = y[:SUB]

    def project(p, first):
        for h in range(kvh):
            att_copy(p, h).wait_recv()
        a = jnp.concatenate([jnp.concatenate([att_at(p, side, h, 1)[...] for side in range(2)], 0)
                             for h in range(heads)], 1)
        for j in range(nh):
            if first:
                wo_copy(2 * j).wait()
                wo_copy(2 * j + 1).wait()
            r = mm(a, wo_v[j])
            for i in range(2):
                n = 2 * j + i
                part = r[:, i * CB:(i + 1) * CB]
                if n < nh:
                    snd[n, both(p)] = part
                    partial_copy(p, n).start()
                else:
                    x_at = jnp.concatenate([x_v[seqs(p), y_col(n - nh)],
                                            x_v[at_rows(nseq + p * SUB, SUB, SUB), y_col(n - nh)]], 0)
                    own[n - nh, both(p)] = part + x_at.astype(F32)

    def forward(h):
        to_far[h].wait_recv()
        pass_on[h].start()

    for d in range(SUB // per):
        forward(d)
        attend(d, 0)
        refill(d)
        for j in range(nh * d, nh * (d + 1)):
            wo_copy(j).start()
    forward(2)
    to_near.wait_recv()
    for i in range(2):
        kv_new_copy(i).wait_recv()
    merge(0, (0, 1, 2), lambda h: pass_on[h].wait_recv())
    forward(3)
    pass_on[3].wait_recv()
    merge(0, (3,))
    project(0, True)

    def one_pass(p, carry):
        def step(d, cc):
            attend(d, p * SUB)

            @pl.when(2 * d + RING < ngrp)
            def _():
                refill(d)
            return cc
        lax.fori_loop(p * (SUB // per), (p + 1) * (SUB // per), step, 0)
        merge(p, tuple(range(kvh)))
        finish(p - 1)
        project(p, False)
        return carry
    lax.fori_loop(1, npass, one_pass, 0)
    finish(npass - 1)

    for p in range(npass):
        for j in range(nh):
            partial_copy(p, j).wait_send()
            for cp in y_copies(p, j):
                cp.wait()
        for h in range(kvh):
            att_copy(p, h).wait_send()
    for n in range(nq):
        q_copy(n).wait_send()
    for i in range(2):
        kv_new_copy(i).wait_send()
    x_send.wait_send()
    to_near.wait_send()
    for h in range(kvh):
        to_far[h].wait_send()
        pass_on[h].wait_send()


def solution(mesh):
    row_axes = ('dp', 'ctx')

    def device_step(hidden, w_q, w_k, w_v, w_o, k_prefix, v_prefix, k_suffix, v_suffix, seq_lens):
        nseq, model = hidden.shape
        npos, kvh, hd = k_prefix.shape
        slots = k_suffix.shape[1]
        heads = w_q.shape[1] // hd
        rows = slots * kvh
        npass, nh = nseq // SUB, model // 4 // CB
        nw = heads * hd // 2 // CB + 2
        hpb = CB // hd
        dims = (nseq, model, heads, kvh, hd, slots)
        hbm = pl.BlockSpec(memory_space=pl.ANY)
        dma = pltpu.SemaphoreType.DMA
        return pl.pallas_call(
            functools.partial(body, dims),
            out_shape=jax.ShapeDtypeStruct((nseq, model), BF16),
            in_specs=[hbm] * 9 + [pl.BlockSpec(memory_space=pltpu.SMEM)],
            out_specs=pl.BlockSpec(memory_space=pltpu.VMEM),
            scratch_shapes=[
                pltpu.VMEM((2 * nseq, model), BF16),
                pltpu.VMEM((nw, model, CB), BF16),
                pltpu.VMEM((nh, heads * hd, 2 * CB), BF16),
                pltpu.VMEM((RING, GRP * rows, hd), BF16),
                pltpu.VMEM((RING, GRP * rows, hd), BF16),
                pltpu.VMEM((nseq * PAD, hd), F32),
                pltpu.VMEM((heads, nseq, hd), BF16),
                pltpu.VMEM((heads // 2, nseq, hd), BF16),
                pltpu.VMEM((2, kvh, nseq, hd), BF16),
                pltpu.VMEM((2, hpb, nseq, hd), BF16),
                pltpu.VMEM((4, kvh, 2, npos, hd), BF16),
                pltpu.VMEM((PAD, rows), jnp.int32),
                pltpu.VMEM((SUB * PAD, hd), F32),
                pltpu.VMEM((SUB * PAD, hd), F32),
                pltpu.VMEM((nh, 2 * nseq, CB), F32),
                pltpu.VMEM((nh, 2 * nseq, CB), F32),
                pltpu.VMEM((nh, 2 * nseq, CB), F32),
                dma((3,)), dma((2,)), dma((2,)), dma((nw,)), dma((2 * nh,)), dma((RING, 2)),
                dma((2, kvh)), dma((2, kvh)), dma((nw,)), dma((nw,)), dma((npass, kvh)), dma((npass, kvh)),
                dma((npass, nh)), dma((npass, nh)), dma((3, npass, nh)), dma((3, npass, nh)),
            ],
            compiler_params=pltpu.CompilerParams(collective_id=0, has_side_effects=True,
                                                 vmem_limit_bytes=67043328),
        )(hidden, w_q, w_k, w_v, w_o,
          k_prefix.reshape(npos * kvh, hd), v_prefix.reshape(npos * kvh, hd),
          k_suffix.reshape(nseq * rows, hd), v_suffix.reshape(nseq * rows, hd), seq_lens)

    spec_in = (P(row_axes, None), P(None, 'tp'), P(None, 'tp'), P(None, 'tp'), P('tp', None), P(row_axes, 'tp', None), P(row_axes, 'tp', None), P(row_axes, None, 'tp', None), P(row_axes, None, 'tp', None), P(row_axes))
    return jax.shard_map(device_step, mesh=mesh, in_specs=spec_in, out_specs=P(row_axes, None), check_vma=False)
```

```python
import functools

import jax
import jax.numpy as jnp
from jax import lax
from jax.experimental import pallas as pl
from jax.experimental.pallas import tpu as pltpu
from jax.sharding import PartitionSpec as P

MESH = pl.DeviceIdType.MESH
F32 = jnp.float32
BF16 = jnp.bfloat16
LOG2E = 1.4426950408889634
LOW = -3.0e38

CB = 256
SUB = 32
GRP = 8
RING = 4
AHEAD = 3
EARLY = ((0,), (1, 2), (3, 4))
PAD = 24


def mm(a, b):
    return jnp.dot(a, b, preferred_element_type=F32)


def mmt(a, b):
    return lax.dot_general(a, b, (((1,), (1,)), ((), ())), preferred_element_type=F32)


def body(dims, hid, wq, wk, wv, wo, kp, vp, ks, vs, lens, out,
         x_v, w_v, wo_v, k_ring, v_ring, q2, qg, qs, kvn, kvs, kvp, key,
         o2, m2, snd, rcv, own,
         x_sem, p_sem, n_sem, w_sem, wo_sem, kv_sem, g_snd, g_rcv, q_snd, q_rcv, a_snd, a_rcv,
         f_snd, f_rcv, y_snd, y_rcv):
    nseq, model, heads, kvh, hd, slots = dims
    grp_heads = heads // kvh
    rows = slots * kvh
    half = model // 2
    quart = half // 2
    nq = heads * hd // 2 // CB
    nw = nq + 2
    nh = quart // CB
    ngrp = nseq // GRP
    npass = nseq // SUB
    npos = kvp.shape[3]
    c = lax.axis_index('ctx')
    t = lax.axis_index('tp')
    core = lax.rem(c, 2)
    sib = c + 1 - 2 * core
    far = {'ctx': lax.rem(c + 2, 4)}
    near = {'ctx': sib}
    mate = {'tp': 1 - t}
    diag = {'tp': 1 - t, 'ctx': sib}
    cs = LOG2E * hd ** -0.5

    def remote(src, dst, ss, rs, dev):
        return pltpu.make_async_remote_copy(src_ref=src, dst_ref=dst, send_sem=ss, recv_sem=rs,
                                            device_id=dev, device_id_type=MESH)

    def w_copy(n):
        if n < nq:
            src, col = wq, core * (nq * CB) + n * CB
        else:
            src, col = (wk, wv)[n - nq], core * CB
        return pltpu.make_async_copy(src.at[:, pl.ds(pl.multiple_of(col, CB), CB)], w_v.at[n], w_sem.at[n])

    def wo_copy(j):
        side = (1 - t) if j < nh else t
        col = side * half + core * quart + (j % nh) * CB
        return pltpu.make_async_copy(wo.at[:, pl.ds(pl.multiple_of(col, CB), CB)],
                                     wo_v.at[j // 2, :, pl.ds(j % 2 * CB, CB)], wo_sem.at[j])

    def kv_copies(g):
        slot = lax.rem(g, RING)
        src = pl.ds(g * GRP * rows, GRP * rows)
        return [pltpu.make_async_copy(ks.at[src], k_ring.at[slot], kv_sem.at[slot, 0]),
                pltpu.make_async_copy(vs.at[src], v_ring.at[slot], kv_sem.at[slot, 1])]

    def kv_start(g):
        for cp in kv_copies(g):
            cp.start()

    pre = [k_ring.at[RING - 1, pl.ds(0, npos * kvh)], v_ring.at[RING - 1, pl.ds(0, npos * kvh)]]
    x_copy = pltpu.make_async_copy(hid, x_v.at[pl.ds(0, nseq)], x_sem.at[0])
    p_copies = [pltpu.make_async_copy(kp, pre[0], p_sem.at[0]), pltpu.make_async_copy(vp, pre[1], p_sem.at[1])]

    barrier = pltpu.get_barrier_semaphore()
    for dev in (near, far, mate, diag):
        pl.semaphore_signal(barrier, inc=1, device_id=dev, device_id_type=MESH)
    p_copies[0].start()
    p_copies[1].start()
    x_copy.start()
    for n in range(AHEAD):
        w_copy(n).start()

    dei = q2.at[pl.ds(0, npos * kvh)]
    for i in range(2):
        p_copies[i].wait()
        dei[...] = pre[i][...].astype(F32)
        for h in range(kvh):
            kvp[0, h, i] = dei[pl.ds(h, npos, stride=kvh), :].astype(BF16)
    to_far = [remote(kvp.at[0, h], kvp.at[2, h], g_snd.at[0, h], g_rcv.at[0, h], far) for h in range(kvh)]
    pass_on = [remote(kvp.at[2, h], kvp.at[3, h], g_snd.at[1, h], g_rcv.at[1, h], near) for h in range(kvh)]
    to_near = remote(kvp.at[0], kvp.at[1], n_sem.at[0], n_sem.at[1], near)
    x_send = remote(x_v.at[pl.ds(0, nseq)], x_v.at[pl.ds(nseq, nseq)], x_sem.at[1], x_sem.at[2], near)
    x_copy.wait()
    pl.semaphore_wait(barrier, 4)
    for cp in to_far:
        cp.start()
    x_send.start()

    row_head = lax.broadcasted_iota(jnp.int32, (PAD, rows), 0) // grp_heads
    col_row = lax.broadcasted_iota(jnp.int32, (PAD, rows), 1)
    key[...] = jnp.where(lax.rem(col_row, kvh) == row_head, col_row // kvh, slots)
    for h in range(heads, PAD):
        q2[pl.ds(h, nseq, stride=PAD), :] = jnp.zeros((nseq, hd), F32)

    hpb = CB // hd
    mine = core * (nq * hpb)
    theirs = (1 - core) * (nq * hpb)

    def q_copy(n):
        at = pl.ds(hpb * n, hpb)
        return remote(qs.at[at], qg.at[pl.ds(mine + hpb * n, hpb)], q_snd.at[n], q_rcv.at[n], near)

    def kv_new_copy(i):
        return remote(kvs.at[i], kvn.at[i, pl.ds(core * hpb, hpb)], q_snd.at[nq + i], q_rcv.at[nq + i], near)

    def block_dot(lo, n):
        return mm(x_v[lo:lo + nseq], w_v[n]).astype(BF16)

    def put_own(n, r):
        for i in range(hpb):
            one = r[:, i * hd:(i + 1) * hd]
            if n < nq:
                h = mine + hpb * n + i
                qg[h] = one
                q2[pl.ds(h, nseq, stride=PAD), :] = one.astype(F32)
            else:
                kvn[n - nq, core * hpb + i] = one

    def put_other(n, r):
        for i in range(hpb):
            one = r[:, i * hd:(i + 1) * hd]
            if n < nq:
                qs[hpb * n + i] = one
            else:
                kvs[n - nq, i] = one
        if n < nq:
            q_copy(n).start()
        else:
            kv_new_copy(n - nq).start()

    todo = [(0, n) for n in range(nw)] + [(nseq, n) for n in range(nw)]
    for i in range(0, len(todo), 2):
        pair = todo[i:i + 2]
        for lo, n in pair:
            if lo == 0:
                w_copy(n).wait()
                if n + AHEAD < nw:
                    w_copy(n + AHEAD).start()
                else:
                    kv_start(n + AHEAD - nw)
            elif n == 0:
                x_send.wait_recv()
        r = [block_dot(lo, n) for lo, n in pair]
        for (lo, n), one in zip(pair, r):
            (put_other if lo else put_own)(n, one)
    kv_start(RING - 1)
    to_near.start()
    for n in range(nq):
        q_copy(n).wait_recv()
        for i in range(hpb):
            h = theirs + hpb * n + i
            q2[pl.ds(h, nseq, stride=PAD), :] = qg[h].astype(F32)

    zero8 = jnp.zeros((8, hd), F32)
    zero32 = jnp.zeros((32, hd), BF16)
    quarter = rows // 4

    def scores(slot, b, base):
        q = q2[pl.ds(pl.multiple_of(b * PAD, 8), PAD), :]
        q = jnp.concatenate([q, zero8], 0).astype(BF16)
        lhs = jnp.concatenate([jnp.concatenate([q, zero32], 1), jnp.concatenate([zero32, q], 1)], 0)
        s = []
        for p in range(2):
            k0 = k_ring[slot, base + 2 * p * quarter:base + (2 * p + 1) * quarter, :]
            k1 = k_ring[slot, base + (2 * p + 1) * quarter:base + (2 * p + 2) * quarter, :]
            r = mmt(lhs, jnp.concatenate([k0, k1], 1))
            s += [r[0:PAD], r[32:32 + PAD]]
        return s

    def weights(s, b):
        n_old = lens[b]
        s = [jnp.where(key[:, p * quarter:(p + 1) * quarter] < n_old, s[p], -jnp.inf) for p in range(4)]
        m = jnp.maximum(jnp.maximum(s[0], s[1]), jnp.maximum(s[2], s[3]))
        m = jnp.maximum(jnp.max(m, axis=1, keepdims=True), LOW)
        e = [jnp.exp2((a - m) * cs) for a in s]
        l = jnp.sum((e[0] + e[1]) + (e[2] + e[3]), axis=1, keepdims=True)
        gap = jnp.zeros((8, 2 * quarter), F32)
        w = jnp.concatenate([jnp.concatenate([e[0], e[2]], 1), gap,
                             jnp.concatenate([e[1], e[3]], 1), gap], 0).astype(BF16)
        return w, m, l

    def values(w, m, l, slot, base, local):
        v = [v_ring[slot, base + p * quarter:base + (p + 1) * quarter, :] for p in range(4)]
        v = jnp.concatenate([jnp.concatenate([v[0], v[1]], 1), jnp.concatenate([v[2], v[3]], 1)], 0)
        o = mm(w, v)
        at = pl.ds(pl.multiple_of(local * PAD, 8), PAD)
        o2[at, :] = (o[0:PAD, :hd] + o[32:32 + PAD, hd:]) / jnp.maximum(l, 1.0)
        m2[at, :] = jnp.broadcast_to(m + jnp.log2(l) / cs, (PAD, hd))

    per = 2 * GRP

    def attend(d, first):
        for i in range(2):
            for cp in kv_copies(2 * d + i):
                cp.wait()
        slots_of = [lax.rem(2 * d + i, RING) for i in range(2)]
        s, w = {}, {}
        for n in range(per + 2):
            if n < per:
                s[n] = scores(slots_of[n // GRP], d * per + n, n % GRP * rows)
            if 0 <= n - 2 < per:
                m = n - 2
                values(*w.pop(m), slots_of[m // GRP], m % GRP * rows, d * per + m - first)
            if 0 <= n - 1 < per:
                w[n - 1] = weights(s.pop(n - 1), d * per + n - 1)

    def refill(d):
        for i in range(2):
            kv_start(2 * d + RING + i)

    ybuf = w_v.at[0]

    def at_rows(lo, step, size):
        return pl.ds(lo if isinstance(lo, int) else pl.multiple_of(lo, step), size)

    def att_at(p, side, h, count):
        lo = 2 * p * SUB * heads + (side * heads + h) * SUB
        return w_v.at[1, at_rows(lo, SUB, count * SUB), pl.ds(0, hd)]

    def seqs(p):
        return at_rows(p * SUB, SUB, SUB)

    def both(p):
        return at_rows(2 * p * SUB, 2 * SUB, 2 * SUB)

    def y_rows(p, j, side, count):
        return at_rows(2 * (j * nseq + p * SUB) + side * SUB, SUB, count * SUB)

    def merge(p, some, before=lambda h: None):
        size = SUB
        at = seqs(p)

        def pre_scores(h):
            q = qg[h * grp_heads:(h + 1) * grp_heads, at, :].reshape(grp_heads * size, hd)
            return q, [mmt(q, kvp[n, h, 0]) for n in range(4)]

        def pre_weights(sc):
            m = jnp.maximum(jnp.maximum(sc[0], sc[1]), jnp.maximum(sc[2], sc[3]))
            m = jnp.max(m, axis=1, keepdims=True)
            e = [jnp.exp2((a - m) * cs) for a in sc]
            l = jnp.sum((e[0] + e[1]) + (e[2] + e[3]), axis=1, keepdims=True)
            return jnp.concatenate([a.astype(BF16) for a in e], 1), m, l

        def join(h, q, w, m, l):
            o = mm(w, jnp.concatenate([kvp[n, h, 1] for n in range(4)], 0))
            k_new = kvn[0, h, at, :].astype(F32)
            v_new = kvn[1, h, at, :].astype(F32)
            for i in range(grp_heads):
                part = slice(i * size, (i + 1) * size)
                rows_at = pl.ds(h * grp_heads + i, size, stride=PAD)
                m_s, o_s = m2[rows_at, :], o2[rows_at, :]
                s_n = jnp.sum(q[part].astype(F32) * k_new, axis=1, keepdims=True)
                m_p = jnp.maximum(m[part], s_n)
                m_all = jnp.maximum(m_p, m_s)
                w_p = jnp.exp2((m[part] - m_all) * cs)
                w_n = jnp.exp2((s_n - m_all) * cs)
                w_s = jnp.exp2((m_s - m_all) * cs)
                total = w_p * l[part] + w_n + w_s
                val = (w_p * o[part] + w_n * v_new + w_s * o_s) / total
                att_at(p, 0, h * grp_heads + i, 1)[...] = val.astype(BF16)

        sc, w = {}, {}
        for n in range(len(some) + 2):
            if n < len(some):
                before(some[n])
                sc[n] = pre_scores(some[n])
            if 0 <= n - 2:
                join(some[n - 2], *w.pop(n - 2))
                att_copy(p, some[n - 2]).start()
            if 0 <= n - 1 < len(some):
                q, part = sc.pop(n - 1)
                w[n - 1] = (q,) + pre_weights(part)

    def att_copy(p, h):
        mine_at, theirs_at = [att_at(p, side, h * grp_heads, grp_heads) for side in range(2)]
        return remote(mine_at, theirs_at, a_snd.at[p, h], a_rcv.at[p, h], near)

    def partial_copy(p, j):
        return remote(snd.at[j, both(p)], rcv.at[j, both(p)], f_snd.at[p, j], f_rcv.at[p, j], mate)

    def y_col(j):
        return pl.ds(pl.multiple_of(t * half + core * quart + j * CB, CB), CB)

    def y_copies(p, j):
        there = out.at[seqs(p), y_col(j)]
        one, other = [ybuf.at[y_rows(p, j, side, 1)] for side in range(2)]
        return [remote(one, there, y_snd.at[0, p, j], y_rcv.at[0, p, j], mate),
                remote(other, there, y_snd.at[1, p, j], y_rcv.at[1, p, j], diag),
                remote(other, there, y_snd.at[2, p, j], y_rcv.at[2, p, j], near)]

    def finish(p, blocks):
        for j in blocks:
            partial_copy(p, j).wait_recv()
            y = (own[j, both(p)] + rcv[j, both(p)]).astype(BF16)
            ybuf[y_rows(p, j, 0, 2)] = y
            for cp in y_copies(p, j):
                cp.start()
            out[seqs(p), y_col(j)] = y[:SUB]

    def project(p, first):
        for h in range(kvh):
            att_copy(p, h).wait_recv()
        a = jnp.concatenate([jnp.concatenate([att_at(p, side, h, 1)[...] for side in range(2)], 0)
                             for h in range(heads)], 1)
        for j in range(nh):
            if first:
                wo_copy(2 * j).wait()
                wo_copy(2 * j + 1).wait()
            r = mm(a, wo_v[j])
            for i in range(2):
                n = 2 * j + i
                part = r[:, i * CB:(i + 1) * CB]
                if n < nh:
                    snd[n, both(p)] = part
                    partial_copy(p, n).start()
                else:
                    x_at = jnp.concatenate([x_v[seqs(p), y_col(n - nh)],
                                            x_v[at_rows(nseq + p * SUB, SUB, SUB), y_col(n - nh)]], 0)
                    own[n - nh, both(p)] = part + x_at.astype(F32)

    def forward(h):
        to_far[h].wait_recv()
        pass_on[h].start()

    for d in range(SUB // per):
        forward(d)
        attend(d, 0)
        refill(d)
        for j in range(nh * d, nh * (d + 1)):
            wo_copy(j).start()
    forward(2)
    to_near.wait_recv()
    for i in range(2):
        kv_new_copy(i).wait_recv()
    merge(0, (0, 1, 2), lambda h: pass_on[h].wait_recv())
    forward(3)
    pass_on[3].wait_recv()
    merge(0, (3,))
    project(0, True)

    dgs = SUB // per

    def one_pass(p, carry):
        def step(d, cc):
            attend(d, p * SUB)

            @pl.when(2 * d + RING < ngrp)
            def _():
                refill(d)

            @pl.when(d == p * dgs)
            def _():
                finish(p - 1, EARLY[0])

            @pl.when(d == p * dgs + 1)
            def _():
                finish(p - 1, EARLY[1])
            return cc
        lax.fori_loop(p * dgs, (p + 1) * dgs, step, 0)
        merge(p, tuple(range(kvh)))
        finish(p - 1, EARLY[2])
        project(p, False)
        return carry
    lax.fori_loop(1, npass, one_pass, 0)
    finish(npass - 1, range(nh))

    for p in range(npass):
        for j in range(nh):
            partial_copy(p, j).wait_send()
            for cp in y_copies(p, j):
                cp.wait()
        for h in range(kvh):
            att_copy(p, h).wait_send()
    for n in range(nq):
        q_copy(n).wait_send()
    for i in range(2):
        kv_new_copy(i).wait_send()
    x_send.wait_send()
    to_near.wait_send()
    for h in range(kvh):
        to_far[h].wait_send()
        pass_on[h].wait_send()


def solution(mesh):
    row_axes = ('dp', 'ctx')

    def device_step(hidden, w_q, w_k, w_v, w_o, k_prefix, v_prefix, k_suffix, v_suffix, seq_lens):
        nseq, model = hidden.shape
        npos, kvh, hd = k_prefix.shape
        slots = k_suffix.shape[1]
        heads = w_q.shape[1] // hd
        rows = slots * kvh
        npass, nh = nseq // SUB, model // 4 // CB
        nw = heads * hd // 2 // CB + 2
        hpb = CB // hd
        dims = (nseq, model, heads, kvh, hd, slots)
        hbm = pl.BlockSpec(memory_space=pl.ANY)
        dma = pltpu.SemaphoreType.DMA
        return pl.pallas_call(
            functools.partial(body, dims),
            out_shape=jax.ShapeDtypeStruct((nseq, model), BF16),
            in_specs=[hbm] * 9 + [pl.BlockSpec(memory_space=pltpu.SMEM)],
            out_specs=pl.BlockSpec(memory_space=pltpu.VMEM),
            scratch_shapes=[
                pltpu.VMEM((2 * nseq, model), BF16),
                pltpu.VMEM((nw, model, CB), BF16),
                pltpu.VMEM((nh, heads * hd, 2 * CB), BF16),
                pltpu.VMEM((RING, GRP * rows, hd), BF16),
                pltpu.VMEM((RING, GRP * rows, hd), BF16),
                pltpu.VMEM((nseq * PAD, hd), F32),
                pltpu.VMEM((heads, nseq, hd), BF16),
                pltpu.VMEM((heads // 2, nseq, hd), BF16),
                pltpu.VMEM((2, kvh, nseq, hd), BF16),
                pltpu.VMEM((2, hpb, nseq, hd), BF16),
                pltpu.VMEM((4, kvh, 2, npos, hd), BF16),
                pltpu.VMEM((PAD, rows), jnp.int32),
                pltpu.VMEM((SUB * PAD, hd), F32),
                pltpu.VMEM((SUB * PAD, hd), F32),
                pltpu.VMEM((nh, 2 * nseq, CB), F32),
                pltpu.VMEM((nh, 2 * nseq, CB), F32),
                pltpu.VMEM((nh, 2 * nseq, CB), F32),
                dma((3,)), dma((2,)), dma((2,)), dma((nw,)), dma((2 * nh,)), dma((RING, 2)),
                dma((2, kvh)), dma((2, kvh)), dma((nw,)), dma((nw,)), dma((npass, kvh)), dma((npass, kvh)),
                dma((npass, nh)), dma((npass, nh)), dma((3, npass, nh)), dma((3, npass, nh)),
            ],
            compiler_params=pltpu.CompilerParams(collective_id=0, has_side_effects=True,
                                                 vmem_limit_bytes=67043328),
        )(hidden, w_q, w_k, w_v, w_o,
          k_prefix.reshape(npos * kvh, hd), v_prefix.reshape(npos * kvh, hd),
          k_suffix.reshape(nseq * rows, hd), v_suffix.reshape(nseq * rows, hd), seq_lens)

    spec_in = (P(row_axes, None), P(None, 'tp'), P(None, 'tp'), P(None, 'tp'), P('tp', None), P(row_axes, 'tp', None), P(row_axes, 'tp', None), P(row_axes, None, 'tp', None), P(row_axes, None, 'tp', None), P(row_axes))
    return jax.shard_map(device_step, mesh=mesh, in_specs=spec_in, out_specs=P(row_axes, None), check_vma=False)
```

```python
import functools

import jax
import jax.numpy as jnp
from jax import lax
from jax.experimental import pallas as pl
from jax.experimental.pallas import tpu as pltpu
from jax.sharding import PartitionSpec as P

MESH = pl.DeviceIdType.MESH
F32 = jnp.float32
BF16 = jnp.bfloat16
LOG2E = 1.4426950408889634
LOW = -3.0e38

CB = 256
SUB = 32
GRP = 8
RING = 4
AHEAD = 3
EARLY = ((0,), (1, 2), (3, 4))
PAD = 24


def mm(a, b):
    return jnp.dot(a, b, preferred_element_type=F32)


def mmt(a, b):
    return lax.dot_general(a, b, (((1,), (1,)), ((), ())), preferred_element_type=F32)


def body(dims, hid, wq, wk, wv, wo, kp, vp, ks, vs, lens, out,
         x_v, w_v, wo_v, k_ring, v_ring, q2, qg, qs, kvn, kvs, kvp, key,
         o2, m2, snd, rcv, own, out_v, out_sem,
         x_sem, p_sem, n_sem, w_sem, wo_sem, kv_sem, g_snd, g_rcv, q_snd, q_rcv, a_snd, a_rcv,
         f_snd, f_rcv, y_snd, y_rcv):
    nseq, model, heads, kvh, hd, slots = dims
    grp_heads = heads // kvh
    rows = slots * kvh
    half = model // 2
    quart = half // 2
    nq = heads * hd // 2 // CB
    nw = nq + 2
    nh = quart // CB
    ngrp = nseq // GRP
    npass = nseq // SUB
    npos = kvp.shape[3]
    c = lax.axis_index('ctx')
    t = lax.axis_index('tp')
    core = lax.rem(c, 2)
    sib = c + 1 - 2 * core
    far = {'ctx': lax.rem(c + 2, 4)}
    near = {'ctx': sib}
    mate = {'tp': 1 - t}
    diag = {'tp': 1 - t, 'ctx': sib}
    cs = LOG2E * hd ** -0.5

    def remote(src, dst, ss, rs, dev):
        return pltpu.make_async_remote_copy(src_ref=src, dst_ref=dst, send_sem=ss, recv_sem=rs,
                                            device_id=dev, device_id_type=MESH)

    def w_copy(n):
        if n < nq:
            src, col = wq, core * (nq * CB) + n * CB
        else:
            src, col = (wk, wv)[n - nq], core * CB
        return pltpu.make_async_copy(src.at[:, pl.ds(pl.multiple_of(col, CB), CB)], w_v.at[n], w_sem.at[n])

    def wo_copy(j):
        side = (1 - t) if j < nh else t
        col = side * half + core * quart + (j % nh) * CB
        return pltpu.make_async_copy(wo.at[:, pl.ds(pl.multiple_of(col, CB), CB)],
                                     wo_v.at[j // 2, :, pl.ds(j % 2 * CB, CB)], wo_sem.at[j])

    def kv_copies(g):
        slot = lax.rem(g, RING)
        src = pl.ds(g * GRP * rows, GRP * rows)
        return [pltpu.make_async_copy(ks.at[src], k_ring.at[slot], kv_sem.at[slot, 0]),
                pltpu.make_async_copy(vs.at[src], v_ring.at[slot], kv_sem.at[slot, 1])]

    def kv_start(g):
        for cp in kv_copies(g):
            cp.start()

    pre = [k_ring.at[RING - 1, pl.ds(0, npos * kvh)], v_ring.at[RING - 1, pl.ds(0, npos * kvh)]]
    x_copy = pltpu.make_async_copy(hid, x_v.at[pl.ds(0, nseq)], x_sem.at[0])
    p_copies = [pltpu.make_async_copy(kp, pre[0], p_sem.at[0]), pltpu.make_async_copy(vp, pre[1], p_sem.at[1])]

    barrier = pltpu.get_barrier_semaphore()
    for dev in (near, far, mate, diag):
        pl.semaphore_signal(barrier, inc=1, device_id=dev, device_id_type=MESH)
    p_copies[0].start()
    p_copies[1].start()
    x_copy.start()
    for n in range(AHEAD):
        w_copy(n).start()

    dei = q2.at[pl.ds(0, npos * kvh)]
    for i in range(2):
        p_copies[i].wait()
        dei[...] = pre[i][...].astype(F32)
        for h in range(kvh):
            kvp[0, h, i] = dei[pl.ds(h, npos, stride=kvh), :].astype(BF16)
    to_far = [remote(kvp.at[0, h], kvp.at[2, h], g_snd.at[0, h], g_rcv.at[0, h], far) for h in range(kvh)]
    pass_on = [remote(kvp.at[2, h], kvp.at[3, h], g_snd.at[1, h], g_rcv.at[1, h], near) for h in range(kvh)]
    to_near = remote(kvp.at[0], kvp.at[1], n_sem.at[0], n_sem.at[1], near)
    x_send = remote(x_v.at[pl.ds(0, nseq)], x_v.at[pl.ds(nseq, nseq)], x_sem.at[1], x_sem.at[2], near)
    x_copy.wait()
    pl.semaphore_wait(barrier, 4)
    for cp in to_far:
        cp.start()
    x_send.start()

    row_head = lax.broadcasted_iota(jnp.int32, (PAD, rows), 0) // grp_heads
    col_row = lax.broadcasted_iota(jnp.int32, (PAD, rows), 1)
    key[...] = jnp.where(lax.rem(col_row, kvh) == row_head, col_row // kvh, slots)
    for h in range(heads, PAD):
        q2[pl.ds(h, nseq, stride=PAD), :] = jnp.zeros((nseq, hd), F32)

    hpb = CB // hd
    mine = core * (nq * hpb)
    theirs = (1 - core) * (nq * hpb)

    def q_copy(n):
        at = pl.ds(hpb * n, hpb)
        return remote(qs.at[at], qg.at[pl.ds(mine + hpb * n, hpb)], q_snd.at[n], q_rcv.at[n], near)

    def kv_new_copy(i):
        return remote(kvs.at[i], kvn.at[i, pl.ds(core * hpb, hpb)], q_snd.at[nq + i], q_rcv.at[nq + i], near)

    def block_dot(lo, n):
        return mm(x_v[lo:lo + nseq], w_v[n]).astype(BF16)

    def put_own(n, r):
        for i in range(hpb):
            one = r[:, i * hd:(i + 1) * hd]
            if n < nq:
                h = mine + hpb * n + i
                qg[h] = one
                q2[pl.ds(h, nseq, stride=PAD), :] = one.astype(F32)
            else:
                kvn[n - nq, core * hpb + i] = one

    def put_other(n, r):
        for i in range(hpb):
            one = r[:, i * hd:(i + 1) * hd]
            if n < nq:
                qs[hpb * n + i] = one
            else:
                kvs[n - nq, i] = one
        if n < nq:
            q_copy(n).start()
        else:
            kv_new_copy(n - nq).start()

    order = [(0, range(nq)), (nseq, range(nq)), (0, range(nq, nw)), (nseq, range(nq, nw))]
    todo = [(lo, n) for lo, part in order for n in part]
    for i in range(0, len(todo), 2):
        pair = todo[i:i + 2]
        for lo, n in pair:
            if lo == 0:
                w_copy(n).wait()
                if n + AHEAD < nw:
                    w_copy(n + AHEAD).start()
                else:
                    kv_start(n + AHEAD - nw)
            elif n == 0:
                x_send.wait_recv()
        r = [block_dot(lo, n) for lo, n in pair]
        for (lo, n), one in zip(pair, r):
            (put_other if lo else put_own)(n, one)
    kv_start(RING - 1)
    to_near.start()
    for n in range(nq):
        q_copy(n).wait_recv()
        for i in range(hpb):
            h = theirs + hpb * n + i
            q2[pl.ds(h, nseq, stride=PAD), :] = qg[h].astype(F32)

    zero8 = jnp.zeros((8, hd), F32)
    zero32 = jnp.zeros((32, hd), BF16)
    quarter = rows // 4

    def scores(slot, b, base):
        q = q2[pl.ds(pl.multiple_of(b * PAD, 8), PAD), :]
        q = jnp.concatenate([q, zero8], 0).astype(BF16)
        lhs = jnp.concatenate([jnp.concatenate([q, zero32], 1), jnp.concatenate([zero32, q], 1)], 0)
        s = []
        for p in range(2):
            k0 = k_ring[slot, base + 2 * p * quarter:base + (2 * p + 1) * quarter, :]
            k1 = k_ring[slot, base + (2 * p + 1) * quarter:base + (2 * p + 2) * quarter, :]
            r = mmt(lhs, jnp.concatenate([k0, k1], 1))
            s += [r[0:PAD], r[32:32 + PAD]]
        return s

    def weights(s, b):
        n_old = lens[b]
        s = [jnp.where(key[:, p * quarter:(p + 1) * quarter] < n_old, s[p], -jnp.inf) for p in range(4)]
        m = jnp.maximum(jnp.maximum(s[0], s[1]), jnp.maximum(s[2], s[3]))
        m = jnp.maximum(jnp.max(m, axis=1, keepdims=True), LOW)
        e = [jnp.exp2((a - m) * cs) for a in s]
        l = jnp.sum((e[0] + e[1]) + (e[2] + e[3]), axis=1, keepdims=True)
        gap = jnp.zeros((8, 2 * quarter), F32)
        w = jnp.concatenate([jnp.concatenate([e[0], e[2]], 1), gap,
                             jnp.concatenate([e[1], e[3]], 1), gap], 0).astype(BF16)
        return w, m, l

    def values(w, m, l, slot, base, local):
        v = [v_ring[slot, base + p * quarter:base + (p + 1) * quarter, :] for p in range(4)]
        v = jnp.concatenate([jnp.concatenate([v[0], v[1]], 1), jnp.concatenate([v[2], v[3]], 1)], 0)
        o = mm(w, v)
        at = pl.ds(pl.multiple_of(local * PAD, 8), PAD)
        o2[at, :] = (o[0:PAD, :hd] + o[32:32 + PAD, hd:]) / jnp.maximum(l, 1.0)
        m2[at, :] = jnp.broadcast_to(m + jnp.log2(l) / cs, (PAD, hd))

    per = 2 * GRP

    def attend(d, first):
        for i in range(2):
            for cp in kv_copies(2 * d + i):
                cp.wait()
        slots_of = [lax.rem(2 * d + i, RING) for i in range(2)]
        s, w = {}, {}
        for n in range(per + 2):
            if n < per:
                s[n] = scores(slots_of[n // GRP], d * per + n, n % GRP * rows)
            if 0 <= n - 2 < per:
                m = n - 2
                values(*w.pop(m), slots_of[m // GRP], m % GRP * rows, d * per + m - first)
            if 0 <= n - 1 < per:
                w[n - 1] = weights(s.pop(n - 1), d * per + n - 1)

    def refill(d):
        for i in range(2):
            kv_start(2 * d + RING + i)

    ybuf = w_v.at[0]

    def at_rows(lo, step, size):
        return pl.ds(lo if isinstance(lo, int) else pl.multiple_of(lo, step), size)

    def att_at(p, side, h, count):
        lo = 2 * p * SUB * heads + (side * heads + h) * SUB
        return w_v.at[1, at_rows(lo, SUB, count * SUB), pl.ds(0, hd)]

    def seqs(p):
        return at_rows(p * SUB, SUB, SUB)

    def both(p):
        return at_rows(2 * p * SUB, 2 * SUB, 2 * SUB)

    def y_rows(p, j, side, count):
        return at_rows(2 * (j * nseq + p * SUB) + side * SUB, SUB, count * SUB)

    def merge(p, some, before=lambda h: None):
        size = SUB
        at = seqs(p)

        def pre_scores(h):
            q = qg[h * grp_heads:(h + 1) * grp_heads, at, :].reshape(grp_heads * size, hd)
            return q, [mmt(q, kvp[n, h, 0]) for n in range(4)]

        def pre_weights(sc):
            m = jnp.maximum(jnp.maximum(sc[0], sc[1]), jnp.maximum(sc[2], sc[3]))
            m = jnp.max(m, axis=1, keepdims=True)
            e = [jnp.exp2((a - m) * cs) for a in sc]
            l = jnp.sum((e[0] + e[1]) + (e[2] + e[3]), axis=1, keepdims=True)
            return jnp.concatenate([a.astype(BF16) for a in e], 1), m, l

        def join(h, q, w, m, l):
            o = mm(w, jnp.concatenate([kvp[n, h, 1] for n in range(4)], 0))
            k_new = kvn[0, h, at, :].astype(F32)
            v_new = kvn[1, h, at, :].astype(F32)
            for i in range(grp_heads):
                part = slice(i * size, (i + 1) * size)
                rows_at = pl.ds(h * grp_heads + i, size, stride=PAD)
                m_s, o_s = m2[rows_at, :], o2[rows_at, :]
                s_n = jnp.sum(q[part].astype(F32) * k_new, axis=1, keepdims=True)
                m_p = jnp.maximum(m[part], s_n)
                m_all = jnp.maximum(m_p, m_s)
                w_p = jnp.exp2((m[part] - m_all) * cs)
                w_n = jnp.exp2((s_n - m_all) * cs)
                w_s = jnp.exp2((m_s - m_all) * cs)
                total = w_p * l[part] + w_n + w_s
                val = (w_p * o[part] + w_n * v_new + w_s * o_s) / total
                att_at(p, 0, h * grp_heads + i, 1)[...] = val.astype(BF16)

        sc, w = {}, {}
        for n in range(len(some) + 2):
            if n < len(some):
                before(some[n])
                sc[n] = pre_scores(some[n])
            if 0 <= n - 2:
                join(some[n - 2], *w.pop(n - 2))
                att_copy(p, some[n - 2]).start()
            if 0 <= n - 1 < len(some):
                q, part = sc.pop(n - 1)
                w[n - 1] = (q,) + pre_weights(part)

    def att_copy(p, h):
        mine_at, theirs_at = [att_at(p, side, h * grp_heads, grp_heads) for side in range(2)]
        return remote(mine_at, theirs_at, a_snd.at[p, h], a_rcv.at[p, h], near)

    def partial_copy(p, j):
        return remote(snd.at[j, both(p)], rcv.at[j, both(p)], f_snd.at[p, j], f_rcv.at[p, j], mate)

    def y_col(j):
        return pl.ds(pl.multiple_of(t * half + core * quart + j * CB, CB), CB)

    def y_copies(p, j):
        there = out_v.at[seqs(p), y_col(j)]
        one, other = [ybuf.at[y_rows(p, j, side, 1)] for side in range(2)]
        return [remote(one, there, y_snd.at[0, p, j], y_rcv.at[0, p, j], mate),
                remote(other, there, y_snd.at[1, p, j], y_rcv.at[1, p, j], diag),
                remote(other, there, y_snd.at[2, p, j], y_rcv.at[2, p, j], near)]

    def finish(p, blocks):
        for j in blocks:
            partial_copy(p, j).wait_recv()
            y = (own[j, both(p)] + rcv[j, both(p)]).astype(BF16)
            ybuf[y_rows(p, j, 0, 2)] = y
            for cp in y_copies(p, j):
                cp.start()
            out_v[seqs(p), y_col(j)] = y[:SUB]

    def project(p, first):
        for h in range(kvh):
            att_copy(p, h).wait_recv()
        a = jnp.concatenate([jnp.concatenate([att_at(p, side, h, 1)[...] for side in range(2)], 0)
                             for h in range(heads)], 1)
        for j in range(nh):
            if first:
                wo_copy(2 * j).wait()
                wo_copy(2 * j + 1).wait()
            r = mm(a, wo_v[j])
            for i in range(2):
                n = 2 * j + i
                part = r[:, i * CB:(i + 1) * CB]
                if n < nh:
                    snd[n, both(p)] = part
                    partial_copy(p, n).start()
                else:
                    x_at = jnp.concatenate([x_v[seqs(p), y_col(n - nh)],
                                            x_v[at_rows(nseq + p * SUB, SUB, SUB), y_col(n - nh)]], 0)
                    own[n - nh, both(p)] = part + x_at.astype(F32)

    def forward(h):
        to_far[h].wait_recv()
        pass_on[h].start()

    for d in range(SUB // per):
        forward(d)
        attend(d, 0)
        refill(d)
        for j in range(nh * d, nh * (d + 1)):
            wo_copy(j).start()
    forward(2)
    to_near.wait_recv()
    for i in range(2):
        kv_new_copy(i).wait_recv()
    merge(0, (0, 1, 2), lambda h: pass_on[h].wait_recv())
    forward(3)
    pass_on[3].wait_recv()
    merge(0, (3,))
    project(0, True)

    dgs = SUB // per

    def one_pass(p, carry):
        def step(d, cc):
            attend(d, p * SUB)

            @pl.when(2 * d + RING < ngrp)
            def _():
                refill(d)

            @pl.when(d == p * dgs)
            def _():
                finish(p - 1, EARLY[0])

            @pl.when(d == p * dgs + 1)
            def _():
                finish(p - 1, EARLY[1])
            return cc
        lax.fori_loop(p * dgs, (p + 1) * dgs, step, 0)
        merge(p, tuple(range(kvh)))
        finish(p - 1, EARLY[2])
        project(p, False)
        return carry
    lax.fori_loop(1, npass, one_pass, 0)
    finish(npass - 1, range(nh))

    out_copies = [pltpu.make_async_copy(out_v.at[seqs(p)], out.at[seqs(p)], out_sem.at[p]) for p in range(npass)]
    for p in range(npass):
        for j in range(nh):
            partial_copy(p, j).wait_send()
            for cp in y_copies(p, j):
                cp.wait()
        out_copies[p].start()
        for h in range(kvh):
            att_copy(p, h).wait_send()
    for cp in out_copies:
        cp.wait()
    for n in range(nq):
        q_copy(n).wait_send()
    for i in range(2):
        kv_new_copy(i).wait_send()
    x_send.wait_send()
    to_near.wait_send()
    for h in range(kvh):
        to_far[h].wait_send()
        pass_on[h].wait_send()


def solution(mesh):
    row_axes = ('dp', 'ctx')

    def device_step(hidden, w_q, w_k, w_v, w_o, k_prefix, v_prefix, k_suffix, v_suffix, seq_lens):
        nseq, model = hidden.shape
        npos, kvh, hd = k_prefix.shape
        slots = k_suffix.shape[1]
        heads = w_q.shape[1] // hd
        rows = slots * kvh
        npass, nh = nseq // SUB, model // 4 // CB
        nw = heads * hd // 2 // CB + 2
        hpb = CB // hd
        dims = (nseq, model, heads, kvh, hd, slots)
        hbm = pl.BlockSpec(memory_space=pl.ANY)
        dma = pltpu.SemaphoreType.DMA
        return pl.pallas_call(
            functools.partial(body, dims),
            out_shape=jax.ShapeDtypeStruct((nseq, model), BF16),
            in_specs=[hbm] * 9 + [pl.BlockSpec(memory_space=pltpu.SMEM)],
            out_specs=hbm,
            scratch_shapes=[
                pltpu.VMEM((2 * nseq, model), BF16),
                pltpu.VMEM((nw, model, CB), BF16),
                pltpu.VMEM((nh, heads * hd, 2 * CB), BF16),
                pltpu.VMEM((RING, GRP * rows, hd), BF16),
                pltpu.VMEM((RING, GRP * rows, hd), BF16),
                pltpu.VMEM((nseq * PAD, hd), F32),
                pltpu.VMEM((heads, nseq, hd), BF16),
                pltpu.VMEM((heads // 2, nseq, hd), BF16),
                pltpu.VMEM((2, kvh, nseq, hd), BF16),
                pltpu.VMEM((2, hpb, nseq, hd), BF16),
                pltpu.VMEM((4, kvh, 2, npos, hd), BF16),
                pltpu.VMEM((PAD, rows), jnp.int32),
                pltpu.VMEM((SUB * PAD, hd), F32),
                pltpu.VMEM((SUB * PAD, hd), F32),
                pltpu.VMEM((nh, 2 * nseq, CB), F32),
                pltpu.VMEM((nh, 2 * nseq, CB), F32),
                pltpu.VMEM((nh, 2 * nseq, CB), F32),
                pltpu.VMEM((nseq, model), BF16), dma((npass,)),
                dma((3,)), dma((2,)), dma((2,)), dma((nw,)), dma((2 * nh,)), dma((RING, 2)),
                dma((2, kvh)), dma((2, kvh)), dma((nw,)), dma((nw,)), dma((npass, kvh)), dma((npass, kvh)),
                dma((npass, nh)), dma((npass, nh)), dma((3, npass, nh)), dma((3, npass, nh)),
            ],
            compiler_params=pltpu.CompilerParams(collective_id=0, has_side_effects=True,
                                                 vmem_limit_bytes=67043328),
        )(hidden, w_q, w_k, w_v, w_o,
          k_prefix.reshape(npos * kvh, hd), v_prefix.reshape(npos * kvh, hd),
          k_suffix.reshape(nseq * rows, hd), v_suffix.reshape(nseq * rows, hd), seq_lens)

    spec_in = (P(row_axes, None), P(None, 'tp'), P(None, 'tp'), P(None, 'tp'), P('tp', None), P(row_axes, 'tp', None), P(row_axes, 'tp', None), P(row_axes, None, 'tp', None), P(row_axes, None, 'tp', None), P(row_axes))
    return jax.shard_map(device_step, mesh=mesh, in_specs=spec_in, out_specs=P(row_axes, None), check_vma=False)
```
